32 devices in a mesh: mem: 8 (over y, x, core), lat: 4 (over z).
Axes of the slice: x: 2, y: 2, z: 4, core: 2. Of those that a mesh axis runs over, the one named last changes fastest.
Arguments:
- state: float32 [8, 641, 8, 160], P('mem', None, 'lat'), may hold values from -6 to 6
- conv_kernel: float32 [25, 641], replicated, may hold values from -1.25 to 1.25
- norm_gain: float32 [641], replicated, may hold values from 0.5 to 1.5
- up_weight: bfloat16 [641, 1282], replicated, may hold values from -0.25 to 0.25
- down_weight: bfloat16 [1282, 641], replicated, may hold values from -0.15625 to 0.15625
- field_head_weight: bfloat16 [641, 72], replicated, may hold values from -0.25 to 0.25
- target: float32 [72, 8, 160], P(None, 'lat'), may hold values from -9 to 9
- field_weight: float32 [72], replicated, may hold values from 0.3 to 3
Outputs:
- loss: float32 [], replicated
- grad_kernel: float32 [25, 641], replicated
- grad_gain: float32 [641], replicated
- grad_up: float32 [641, 1282], replicated
- grad_down: float32 [1282, 641], replicated
- grad_head: float32 [641, 72], replicated
The draws below stay inside these ranges and needn't reach their ends.
All inputs are finite; a program needn't handle non-finite values.
Results may differ from the reference program's by a relative error of at most 0.005.
The reference program's roundings to bfloat16 on the way count: a program that leaves them out, or rounds other values in their place, can miss the bound.
Values may be sent and summed in bfloat16 or wider, within the bound.
No kernel may reach another device: no remote copies, remote signals or barrier semaphores. Data moves between devices by JAX's collectives and lax.ppermute only.
A program may use at most 128 MiB of HBM per device.

```python
import math
import jax
import jax.numpy as jnp
from jax import lax

C = 641
HID = 1282
FIELDS = 72
LON = 160
MEMBERS = 8
NLAT = 8


def level_of(rng, dims, cuts, low, high):
    level = 1.0
    for dim, shards_of in cuts:
        draws = jax.random.uniform(jax.random.fold_in(jax.random.fold_in(rng, 6), dim), (shards_of,), jnp.float32, low / len(cuts), high / len(cuts))
        level = level * jnp.repeat(jnp.exp(draws), dims[dim] // shards_of).reshape((-1,) + (1,) * (len(dims) - 1 - dim))
    return level


def centred(key, dims, spread, most, shards=(), held_as=jnp.bfloat16):
    loudness = level_of(key, dims, shards, -0.22, 0.18) if shards else 1.0
    drawn = jax.random.normal(key, dims, jnp.float32) * spread * loudness
    return jnp.minimum(jnp.maximum(drawn, -most), most).astype(held_as)


def setup_inputs(seed: int = 0) -> dict:
    seeds = jax.random.split(jax.random.key(seed), 9)
    state = centred(seeds[0], (MEMBERS, C, NLAT, LON), 1.0, 6.0, ((0, 8), (2, 4)), jnp.float32)
    conv_kernel = centred(seeds[1], (25, C), 25 ** -0.5, 1.25, (), jnp.float32)
    norm_gain = jnp.clip(1.0 + 0.1 * jax.random.normal(seeds[2], (C,), jnp.float32), 0.5, 1.5)
    up_weight = centred(seeds[3], (C, HID), C ** -0.5, 0.25)
    down_weight = centred(seeds[4], (HID, C), HID ** -0.5, 0.15625)
    field_head_weight = centred(seeds[5], (C, FIELDS), C ** -0.5, 0.25)
    target = centred(seeds[6], (FIELDS, NLAT, LON), 1.5, 9.0, ((1, 4),), jnp.float32)
    field_weight = jnp.clip(jnp.exp(jax.random.uniform(seeds[7], (FIELDS,), jnp.float32, math.log(0.3), math.log(3.0))), 0.3, 3.0)
    return dict(state=state, conv_kernel=conv_kernel, norm_gain=norm_gain, up_weight=up_weight, down_weight=down_weight, field_head_weight=field_head_weight, target=target, field_weight=field_weight)


DELTA = 0.1
EPSILON = 1e-05

def softened_absolute(diff):
    return jnp.sqrt(diff * diff + DELTA * DELTA) - DELTA

def softened_derivative(diff):
    return diff / jnp.sqrt(diff * diff + DELTA * DELTA)

def gelu_parts(before_activation):
    cumul = 0.5 * (1.0 + jax.scipy.special.erf(before_activation / math.sqrt(2.0)))
    density = jnp.exp(-0.5 * before_activation * before_activation) / math.sqrt(2.0 * math.pi)
    return (before_activation * cumul, cumul + before_activation * density)

def leading_product(left, right):
    return lax.dot_general(left, right, (((0,), (0,)), ((), ())), preferred_element_type=jnp.float32)

def tail_dot(left, right):
    return lax.dot_general(left, right, (((1,), (1,)), ((), ())), preferred_element_type=jnp.float32)

def stencil(window, kernel, height):
    result = jnp.zeros((window.shape[0], height, window.shape[2]), jnp.float32)
    for col_off in range(5):
        shifted = jnp.roll(window, 2 - col_off, axis=2)
        for row_off in range(5):
            result = result + kernel[row_off * 5 + col_off][:, None, None] * shifted[:, row_off:row_off + height]
    return result

def kernel_grad(window, upstream, height):
    terms = [None] * 25
    for col_off in range(5):
        shifted = jnp.roll(window, 2 - col_off, axis=2)
        for row_off in range(5):
            terms[row_off * 5 + col_off] = lax.optimization_barrier(jnp.sum(upstream * shifted[:, row_off:row_off + height], axis=(1, 2)))
    return jnp.stack(terms)

def forward_apply(field, window, kernel, gain, up_weight, down_weight, field_head_weight):
    height = field.shape[1]
    channels = field.shape[0]
    summed = (field + stencil(window, kernel, height)).reshape(channels, -1)
    center = summed - lax.optimization_barrier(jnp.mean(summed, axis=0))
    inverse_norm = lax.rsqrt(lax.optimization_barrier(jnp.mean(center * center, axis=0)) + EPSILON)
    normalized_input = center * inverse_norm
    gain_scaled = (normalized_input * gain[:, None]).astype(jnp.bfloat16)
    before_activation = leading_product(up_weight, gain_scaled)
    activ, unused = gelu_parts(before_activation)
    hidden_activation = activ.astype(jnp.bfloat16)
    output = summed + leading_product(down_weight, hidden_activation)
    rounded_values = output.astype(jnp.bfloat16)
    member_prediction = leading_product(field_head_weight, rounded_values)
    return (member_prediction, (normalized_input, inverse_norm, gain_scaled, before_activation, hidden_activation, rounded_values))

def backward(window, stored_residuals, cotangent, kernel, gain, up_weight, down_weight, field_head_weight):
    normalized_input, inverse_norm, gain_scaled, before_activation, hidden_activation, rounded_values = stored_residuals
    height = window.shape[1] - 4
    co_round = cotangent.astype(jnp.bfloat16)
    grad_head = tail_dot(rounded_values, co_round)
    d_output = jnp.dot(field_head_weight, co_round, preferred_element_type=jnp.float32)
    d_round = d_output.astype(jnp.bfloat16)
    grad_down = tail_dot(hidden_activation, d_round)
    d_hidden = jnp.dot(down_weight, d_round, preferred_element_type=jnp.float32)
    unused, slope = gelu_parts(before_activation)
    d_preact = (d_hidden * slope).astype(jnp.bfloat16)
    grad_up = tail_dot(gain_scaled, d_preact)
    d_scaled = jnp.dot(up_weight, d_preact, preferred_element_type=jnp.float32)
    grad_gain = lax.optimization_barrier(jnp.sum(d_scaled * normalized_input, axis=1))
    d_normed = d_scaled * gain[:, None]
    d_summed = d_output + inverse_norm * (d_normed - lax.optimization_barrier(jnp.mean(d_normed, axis=0)) - normalized_input * lax.optimization_barrier(jnp.mean(d_normed * normalized_input, axis=0)))
    upstream = d_summed.reshape(window.shape[0], height, window.shape[2])
    grad_kernel = kernel_grad(window, upstream, height)
    return (grad_kernel, grad_gain, grad_up, grad_down, grad_head)

def pad_rows(field):
    return jnp.pad(field, ((0, 0), (2, 2), (0, 0)))

def reference(state, conv_kernel, norm_gain, up_weight, down_weight, field_head_weight, target, field_weight):

    def apply_member(field):
        return forward_apply(field, pad_rows(field), conv_kernel, norm_gain, up_weight, down_weight, field_head_weight)[0]
    ensemble_predictions = lax.map(apply_member, state)
    observed_target = target.reshape(FIELDS, -1)
    row_index = jnp.arange(NLAT).astype(jnp.float32)
    area = jnp.cos(0.5 * math.pi * ((row_index + 0.5) / NLAT - 1.0))
    latitude_weights = field_weight[:, None] * jnp.repeat(area, LON)[None, :]
    member_states = MEMBERS

    def pairwise_update(loop_carry_state, single_member):
        return (loop_carry_state + lax.optimization_barrier(jnp.sum(softened_absolute(single_member[None] - ensemble_predictions), axis=0)), lax.optimization_barrier(jnp.sum(softened_derivative(single_member[None] - ensemble_predictions), axis=0)))
    pairwise_sum, pairwise_derivatives = lax.scan(pairwise_update, jnp.zeros(observed_target.shape, jnp.float32), ensemble_predictions)
    ensemble_spread = lax.optimization_barrier(jnp.mean(softened_absolute(ensemble_predictions - observed_target[None]), axis=0)) - pairwise_sum / (2.0 * member_states * (member_states - 1))
    member_count = NLAT * LON * FIELDS
    loss = jnp.sum(latitude_weights * ensemble_spread) / member_count
    member_adjoints = latitude_weights[None] * (softened_derivative(ensemble_predictions - observed_target[None]) - pairwise_derivatives / (member_states - 1)) / (member_states * math.sqrt(member_count))

    def grad_step(loop_carry_state, items):
        field, cotangent = items
        window = pad_rows(field)
        unused, stored_residuals = forward_apply(field, window, conv_kernel, norm_gain, up_weight, down_weight, field_head_weight)
        grads = backward(window, stored_residuals, cotangent, conv_kernel, norm_gain, up_weight, down_weight, field_head_weight)
        return (jax.tree.map(jnp.add, loop_carry_state, grads), None)
    start = (jnp.zeros((25, C), jnp.float32), jnp.zeros((C,), jnp.float32), jnp.zeros((C, HID), jnp.float32), jnp.zeros((HID, C), jnp.float32), jnp.zeros((C, FIELDS), jnp.float32))
    totals, unused = lax.scan(grad_step, start, (state, member_adjoints))
    return (loss, totals[0], totals[1], totals[2], totals[3], totals[4])
```

```python
import math

import jax
import jax.numpy as jnp
from jax import lax
from jax.experimental import pallas as pl
from jax.experimental.pallas import tpu as pltpu
from jax.sharding import PartitionSpec as P

DELTA = 0.1
EPSILON = 1e-05
BF = jnp.bfloat16
F32 = jnp.float32


def dot(left, right, dims):
    return lax.dot_general(left, right, (dims, ((), ())), preferred_element_type=F32)


def pick(stack, index):
    return lax.dynamic_index_in_dim(stack, index, 0, keepdims=False)


def swap(value, axis, mask):
    count = lax.axis_size(axis)
    return lax.ppermute(value, axis, [(i, i ^ mask) for i in range(count)])


def stages():
    members = lax.axis_size("mem")
    return (("mem", 1, 2), ("mem", 2, members // 2), ("lat", 1, lax.axis_size("lat")))


def order(size):
    return sorted(range(1, size), key=lambda k: -bin(k).count("1"))


def scatter_sum(value):
    for axis, stride, size in stages():
        place = (lax.axis_index(axis) // stride) % size
        rows = value.shape[0] // size
        blocks = value.reshape(size, rows, value.shape[1])
        parts = [swap(pick(blocks, place ^ k), axis, k * stride) for k in order(size)]
        total = pick(blocks, place).astype(F32)
        for part in parts:
            total = total + part.astype(F32)
        value = total.astype(BF)
    return value


def gather(value):
    for axis, stride, size in reversed(stages()):
        place = (lax.axis_index(axis) // stride) % size
        got = [value] * size
        for k in order(size):
            got[k] = swap(value, axis, k * stride)
        if size == 2:
            value = jnp.where(
                place == 0, jnp.concatenate(got), jnp.concatenate([got[1], got[0]])
            )
        else:
            got = jnp.stack(got)
            value = jnp.concatenate([pick(got, place ^ k) for k in range(size)])
    return value


def call(kernel, outs, args, flops, scratch=(), smem=()):
    spec = pl.BlockSpec(memory_space=pltpu.VMEM)
    size = sum(math.prod(o.shape) * o.dtype.itemsize for o in outs)
    size += sum(math.prod(a.shape) * a.dtype.itemsize for a in args)
    return pl.pallas_call(
        kernel,
        out_shape=outs,
        in_specs=[
            pl.BlockSpec(memory_space=pltpu.SMEM) if n in smem else spec for n in range(len(args))
        ],
        out_specs=[spec] * len(outs),
        scratch_shapes=list(scratch),
        cost_estimate=pl.CostEstimate(flops=flops, bytes_accessed=size, transcendentals=0),
        compiler_params=pltpu.CompilerParams(vmem_limit_bytes=30 * 1024 * 1024),
    )(*args)


def shape(dims, dtype=F32):
    return jax.ShapeDtypeStruct(tuple(dims), dtype)


def spans(total, step):
    count = max(total // step, 1)
    return [(n * step, total if n == count - 1 else (n + 1) * step) for n in range(count)]


def pack_kernel(field_ref, out_ref):
    rows, width, channels = field_ref.shape
    lanes = out_ref.shape[1]
    cells = rows * width
    for r in range(rows):
        out_ref[r * width : (r + 1) * width, :] = field_ref[r, :, :lanes]
    last = jnp.concatenate(
        [
            jnp.broadcast_to(field_ref[r, :, lanes:channels], (width, 128))
            for r in range(rows)
        ]
    )
    out_ref[cells : cells + 8, :] = jnp.zeros((8, lanes), F32)
    out_ref[cells : cells + 8, :cells] = last.T[:8]


def forward_kernel(
    field_ref, above_ref, below_ref, kernel_ref, gain_ref, up_ref, down_ref, head_ref,
    forecast_ref, win_ref, normed_ref, inverse_ref, scaled_ref, turned_ref, hidden_ref,
    slope_ref, rounded_ref, summed_ref,
):
    height, width, channels = field_ref.shape
    lanes = above_ref.shape[1]
    cells = height * width

    def put(row, main, last):
        for columns, value in ((slice(0, lanes), main), (slice(lanes, channels), last)):
            win_ref[row, 8 : 8 + width, columns] = value
            win_ref[row, 6:8, columns] = value[width - 2 :]
            win_ref[row, 8 + width : 10 + width, columns] = value[:2]

    for base, ref in ((0, above_ref), (2 + height, below_ref)):
        turned = ref[2 * width : 2 * width + 8, :].T
        for r in range(2):
            put(
                base + r,
                ref[r * width : (r + 1) * width, :],
                turned[r * width : (r + 1) * width, :1],
            )
    for r in range(height):
        put(2 + r, field_ref[r, :, :lanes], field_ref[r, :, lanes:])

    part = width // 2

    def convolve(columns):
        for half in range(2):
            first = half * part
            acc = [win_ref[i + 2, 8 + first : 8 + first + part, columns] for i in range(height)]
            for w in range(height + 4):
                for b in range(5):
                    moved = win_ref[w, 6 + b + first : 6 + b + first + part, columns]
                    for i in range(height):
                        if 0 <= w - i < 5:
                            t = 5 * (w - i) + b
                            acc[i] = acc[i] + kernel_ref[t : t + 1, columns] * moved
            for i in range(height):
                start = i * width + first
                summed_ref[start : start + part, columns] = acc[i]

    @pl.loop(0, lanes // 128)
    def _(n):
        convolve(pl.ds(pl.multiple_of(n * 128, 128), 128))

    convolve(slice(lanes, channels))

    for start in range(0, cells, part):
        rows = slice(start, start + part)
        summed = summed_ref[rows, :]
        center = summed - jnp.sum(summed, axis=1, keepdims=True) * (1.0 / channels)
        variance = jnp.sum(center * center, axis=1, keepdims=True) * (1.0 / channels)
        inverse = lax.rsqrt(variance + EPSILON)
        normed = center * inverse
        normed_ref[rows, :] = normed
        inverse_ref[rows, :] = inverse
        scaled_ref[rows, :] = (normed * gain_ref[...]).astype(BF)

    turned_ref[...] = scaled_ref[...].T
    output = summed_ref[...]
    for lo, hi in spans(up_ref.shape[1], 256):
        preact = dot(scaled_ref[...], up_ref[:, lo:hi], ((1,), (0,)))
        cumul = 0.5 * (1.0 + lax.erf(preact * (1.0 / math.sqrt(2.0))))
        density = jnp.exp(-0.5 * preact * preact) * (1.0 / math.sqrt(2.0 * math.pi))
        hidden = (preact * cumul).astype(BF)
        hidden_ref[:, lo:hi] = hidden
        slope_ref[:, lo:hi] = cumul + preact * density
        summed_ref[...] += dot(hidden, down_ref[:, lo:hi], ((1,), (1,)))
    rounded = summed_ref[...].astype(BF)
    rounded_ref[...] = rounded
    forecast_ref[...] = dot(head_ref[...], rounded, ((1,), (1,)))


def score_kernel(
    place_ref, forecast_ref, *refs
):
    members = refs[0].shape[0] * 2
    (far_ref, *near_refs) = refs[: members // 2]
    (
        truth_ref, weight_ref, head_ref, down_ref, rounded_ref, hidden_ref, slope_ref, turned_ref,
        main_ref, output_ref, preact_ref, head_term_ref, factor_ref, loss_ref, cot_ref,
    ) = refs[members // 2 :]
    fields, cells = forecast_ref.shape
    lanes = main_ref.shape[1]
    count = place_ref[0, 1].astype(F32)
    forecast = forecast_ref[...]
    weights = weight_ref[...]
    miss = forecast - truth_ref[...]
    pair_abs = jnp.zeros_like(forecast)
    pair_der = jnp.zeros_like(forecast)
    others = [r[...] for r in near_refs] + [far_ref[k] for k in range(members // 2)]
    for other in others:
        diff = forecast - other
        square = diff * diff + DELTA * DELTA
        inverse = lax.rsqrt(square)
        pair_abs = pair_abs + (square * inverse - DELTA)
        pair_der = pair_der + diff * inverse
    square = miss * miss + DELTA * DELTA
    inverse = lax.rsqrt(square)
    spread = (square * inverse - DELTA) * (1.0 / members) - pair_abs * (
        1.0 / (2.0 * members * (members - 1))
    )
    part = jnp.sum(jnp.sum(weights * spread, axis=1, keepdims=True), axis=0, keepdims=True)
    first = part.astype(BF).astype(F32)
    second = (part - first).astype(BF).astype(F32)
    third = part - first - second
    slot = lax.broadcasted_iota(jnp.int32, (8, lanes), 1) == place_ref[0, 0]
    line = lax.broadcasted_iota(jnp.int32, (8, lanes), 0)
    value = jnp.where(line == 0, first, jnp.where(line == 1, second, third))
    loss_ref[...] = jnp.where(slot & (line < 3), value, 0.0)
    cot = (
        weights
        * (miss * inverse - pair_der * (1.0 / (members - 1)))
        * (lax.rsqrt(count) * (1.0 / members))
    )
    co = cot.astype(BF)
    cot_ref[...] = jnp.zeros_like(cot_ref)
    cot_ref[:fields, :cells] = co.astype(F32)
    turned = cot_ref[...].T[:cells, :fields].astype(BF)
    head_term_ref[...] = dot(co, rounded_ref[...], ((1,), (0,)))
    d_output = dot(turned, head_ref[...], ((1,), (0,)))
    output_ref[...] = d_output
    d_round = d_output.astype(BF)
    for lo, hi in spans(down_ref.shape[1], 256):
        factor_ref[:, lo:hi] = dot(co, hidden_ref[:, lo:hi], ((1,), (0,)))
        d_hidden = dot(d_round, down_ref[:, lo:hi], ((1,), (0,)))
        preact_ref[:, lo:hi] = (d_hidden * slope_ref[:, lo:hi]).astype(BF)
    rows = main_ref.shape[0]
    start = 0
    while start < rows:
        h, r = start // lanes, start % lanes
        take = min(lanes - r, rows - start)
        main_ref[start : start + take, :] = dot(
            turned_ref[r : r + take, :], preact_ref[:, h * lanes : (h + 1) * lanes], ((1,), (0,))
        )
        start += take


def rest_kernel(
    preact_ref, turned_ref, scaled_ref, up_ref, gain_ref, normed_ref, inverse_ref, output_ref,
    win_ref, head_term_ref, factor_ref, loss_ref,
    out_ref, wide_ref, grads_ref, heads_ref,
):
    cells, channels = normed_ref.shape
    hidden_units = preact_ref.shape[1]
    fields = head_term_ref.shape[0]
    lanes = out_ref.shape[1]
    halves = hidden_units // lanes
    even = halves * lanes
    height = win_ref.shape[0] - 4
    width = cells // height
    base = out_ref.shape[0] - 256
    start = halves * lanes - base
    row = 0
    while row < base:
        h, r = (start + row) // lanes, (start + row) % lanes
        take = min(lanes - r, base - row)
        out_ref[row : row + take, :] = dot(
            turned_ref[r : r + take, :], preact_ref[:, h * lanes : (h + 1) * lanes], ((1,), (0,))
        )
        row += take

    for h in range(halves):
        at = base + h * fields
        out_ref[at : at + fields, :] = factor_ref[:, h * lanes : (h + 1) * lanes]
    at = base + halves * fields
    out_ref[at : at + fields, :] = head_term_ref[:, :lanes]
    at += fields

    d_scaled = dot(preact_ref[...], up_ref[...], ((1,), (1,)))
    normed = normed_ref[...]
    grads_ref[...] = jnp.zeros_like(grads_ref)
    grads_ref[25:26, :channels] = jnp.sum(d_scaled * normed, axis=0, keepdims=True)
    d_normed = d_scaled * gain_ref[...]
    d_summed = output_ref[...] + inverse_ref[...] * (
        d_normed
        - jnp.sum(d_normed, axis=1, keepdims=True) * (1.0 / channels)
        - normed * (jnp.sum(d_normed * normed, axis=1, keepdims=True) * (1.0 / channels))
    )
    wide_ref[...] = d_summed

    def correlate(columns):
        for a in range(5):
            for b in range(5):
                total = None
                for i in range(height):
                    term = jnp.sum(
                        wide_ref[i * width : (i + 1) * width, columns]
                        * win_ref[i + a, 6 + b : 6 + b + width, columns],
                        axis=0,
                        keepdims=True,
                    )
                    total = term if total is None else total + term
                t = 5 * a + b
                grads_ref[t : t + 1, columns] = total

    @pl.loop(0, lanes // 128)
    def _(n):
        correlate(pl.ds(pl.multiple_of(n * 128, 128), 128))

    correlate(slice(lanes, channels))

    out_ref[at : at + 26, :] = grads_ref[:26, :lanes]
    at += 26
    last = dot(turned_ref[lanes - 7 : channels, :], preact_ref[...], ((1,), (0,)))[7:8]
    for h in range(halves):
        out_ref[at + h : at + h + 1, :] = last[:, h * lanes : (h + 1) * lanes]
    at += halves
    left = hidden_units - even
    columns = dot(preact_ref[:, even:], scaled_ref[...], ((0,), (0,)))
    out_ref[at : at + left, :] = columns[:, :lanes]
    at += left
    out_ref[at:, :] = jnp.zeros((out_ref.shape[0] - at, lanes), F32)
    heads_ref[...] = jnp.zeros_like(heads_ref)
    heads_ref[:fields, :left] = factor_ref[:, even:]
    out_ref[at : at + left, :128] = heads_ref[...].T[:left]
    at += left
    heads_ref[:fields, :1] = head_term_ref[:, lanes:]
    out_ref[at : at + 1, :128] = heads_ref[...].T[:1]
    at += 1
    out_ref[at : at + 1, :128] = grads_ref[:, lanes : lanes + 128].T[:1]
    at += 1
    out_ref[at : at + 1, :left] = last[:, even:]
    at += 1
    out_ref[at : at + 3, :] = loss_ref[:3]


def finish_kernel(
    one_ref, two_ref, head_ref, loss_ref, kernel_ref, gain_ref, up_ref, down_ref, head_out_ref
):
    channels, hidden_units = up_ref.shape
    lanes = one_ref.shape[1]
    fields = head_ref.shape[1]
    taps = kernel_ref.shape[0]
    halves = hidden_units // lanes
    even = halves * lanes
    left = hidden_units - even
    base = two_ref.shape[0] - 256
    rows = 0
    for ref, total in ((one_ref, one_ref.shape[0]), (two_ref, base)):
        at = 0
        while at < total:
            h, r = rows // lanes, rows % lanes
            take = min(lanes - r, total - at)
            up_ref[r : r + take, h * lanes : (h + 1) * lanes] = ref[at : at + take, :].astype(F32)
            rows += take
            at += take
    for h in range(halves):
        down_ref[:, h * lanes : (h + 1) * lanes] = dot(
            head_ref[...], two_ref[base + h * fields : base + (h + 1) * fields, :], ((1,), (0,))
        )
    extra = two_ref[base:, :].astype(F32)
    at = halves * fields
    head_out_ref[:, :lanes] = extra[at : at + fields]
    at += fields
    kernel_ref[:, :lanes] = extra[at : at + taps]
    at += taps
    gain_ref[:, :lanes] = extra[at : at + 1]
    at += 1
    for h in range(halves):
        up_ref[lanes:channels, h * lanes : (h + 1) * lanes] = extra[at + h : at + h + 1]
    at += halves
    tail = extra[240:256].T
    up_ref[:lanes, even:] = tail[:lanes, at - 240 : at - 240 + left]
    at += left
    down_ref[:, even:] = dot(
        head_ref[...], extra[at : at + left, :fields].astype(BF), ((1,), (1,))
    )
    at += left
    head_out_ref[:, lanes:] = tail[:fields, at - 240 : at - 239]
    at += 1
    kernel_ref[:, lanes:] = tail[:taps, at - 240 : at - 239]
    gain_ref[:, lanes:] = extra[at : at + 1, taps : taps + 1]
    at += 1
    up_ref[lanes:channels, even:] = extra[at : at + 1, :left]
    at += 1
    total = extra[at : at + 1] + extra[at + 1 : at + 2] + extra[at + 2 : at + 3]
    loss_ref[...] = jnp.sum(total, axis=1, keepdims=True)


def local(
    state, conv_kernel, norm_gain, up_weight, down_weight, field_head_weight, target, field_weight
):
    members = lax.axis_size("mem")
    bands = lax.axis_size("lat")
    field = jnp.transpose(state[0], (1, 2, 0))
    height, width, channels = field.shape
    cells = height * width
    hidden_units = up_weight.shape[1]
    nlat = bands * height
    nfields = target.shape[0]
    lanes = channels // 128 * 128
    halves = hidden_units // lanes
    down_turned = down_weight.T
    head_turned = field_head_weight.T
    gain = norm_gain[None]

    def halo(first, pairs):
        sent = call(
            pack_kernel, [shape((2 * width + 8, lanes))], (field[first : first + 2],), 1000000
        )[0]
        return lax.ppermute(sent, "lat", pairs)

    above = halo(height - 2, [(i, i + 1) for i in range(bands - 1)])
    below = halo(0, [(i + 1, i) for i in range(bands - 1)])
    row = (lax.axis_index("lat") * height + jnp.arange(height)).astype(F32)
    area = jnp.repeat(jnp.cos(0.5 * math.pi * ((row + 0.5) / nlat - 1.0)), width)
    weights = field_weight[:, None] * area[None, :]
    count = nlat * width * nfields
    mine = lax.axis_index("mem") * bands + lax.axis_index("lat")
    place = jnp.stack([mine, jnp.int32(count)]).astype(jnp.int32)[None]

    mlp = 2 * cells * channels * hidden_units
    forecast, window, normed, inverse, scaled, turned, hidden, slope, rounded = call(
        forward_kernel,
        [
            shape((nfields, cells)),
            shape((height + 4, width + 16, channels)),
            shape((cells, channels)),
            shape((cells, 1)),
            shape((cells, channels), BF),
            shape((channels, cells), BF),
            shape((cells, hidden_units), BF),
            shape((cells, hidden_units)),
            shape((cells, channels), BF),
        ],
        (field, above, below, conv_kernel, gain, up_weight, down_turned, head_turned),
        2 * mlp,
        [pltpu.VMEM((cells, channels), F32)],
    )
    near = [forecast] + [swap(forecast, "mem", 2 * k) for k in order(members // 2)]
    far = swap(jnp.stack(near), "mem", 1)
    truth = target.reshape(nfields, cells)
    main_rows = halves * lanes
    cut = (main_rows + 256) // 2
    main, d_output, d_preact, head_term, factor, loss_rows = call(
        score_kernel,
        [
            shape((cut, lanes)),
            shape((cells, channels)),
            shape((cells, hidden_units), BF),
            shape((nfields, channels)),
            shape((nfields, hidden_units)),
            shape((8, lanes)),
        ],
        (
            place, forecast, far, *near[1:], truth, weights, head_turned, down_turned, rounded,
            hidden, slope, turned,
        ),
        2 * mlp,
        [pltpu.VMEM((128, -(-cells // 128) * 128), F32)],
        smem=(0,),
    )
    (rest,) = call(
        rest_kernel,
        [shape((main_rows + 256 - cut, lanes))],
        (
            d_preact, turned, scaled, up_weight, gain, normed, inverse, d_output, window,
            head_term, factor, loss_rows,
        ),
        2 * mlp,
        [
            pltpu.VMEM((cells, channels), F32),
            pltpu.VMEM((128, lanes + 128), F32),
            pltpu.VMEM((128, 128), F32),
        ],
    )
    one = gather(scatter_sum(main))
    two = gather(scatter_sum(rest))
    loss, grad_kernel, grad_gain, grad_up, grad_down, grad_head = call(
        finish_kernel,
        [
            shape((1, 1)),
            shape(conv_kernel.shape),
            shape((1, channels)),
            shape(up_weight.shape),
            shape((channels, hidden_units)),
            shape((nfields, channels)),
        ],
        (one, two, field_head_weight),
        mlp // 4,
    )[:6]
    return (
        loss[0, 0] / count, grad_kernel, grad_gain[0], grad_up, grad_down.T, grad_head.T,
    )


def solution(mesh):
    return jax.shard_map(
        local,
        mesh=mesh,
        in_specs=(P("mem", None, "lat", None), P(), P(), P(), P(), P(), P(None, "lat", None), P()),
        out_specs=(P(), P(), P(), P(), P(), P()),
        check_vma=False,
    )
```

```python
import functools
import math

import jax
import jax.numpy as jnp
from jax import lax
from jax.experimental import pallas as pl
from jax.experimental.pallas import tpu as pltpu
from jax.sharding import PartitionSpec as P

DELTA = 0.1
EPSILON = 1e-05
BF = jnp.bfloat16
F32 = jnp.float32


def dot(left, right, dims):
    return lax.dot_general(left, right, (dims, ((), ())), preferred_element_type=F32)


def pick(stack, index):
    return lax.dynamic_index_in_dim(stack, index, 0, keepdims=False)


def swap(value, axis, mask):
    count = lax.axis_size(axis)
    return lax.ppermute(value, axis, [(i, i ^ mask) for i in range(count)])


def stages():
    members = lax.axis_size("mem")
    return (("mem", 1, 2), ("mem", 2, members // 2), ("lat", 1, lax.axis_size("lat")))


def order(size):
    return sorted(range(1, size), key=lambda k: -bin(k).count("1"))


def place_on(stage):
    axis, stride, size = stage
    return (lax.axis_index(axis) // stride) % size


def hand_out(stage, pieces_ref, own_ref, sent_refs):
    place = place_on(stage)
    own_ref[...] = pieces_ref[place]
    for k, ref in zip(order(stage[2]), sent_refs):
        ref[...] = pieces_ref[lax.bitwise_xor(place, k)].astype(ref.dtype)


def sum_kernel(stage, count, *refs):
    total = refs[0][...]
    for ref in refs[1:count]:
        total = total + ref[...].astype(F32)
    if stage is None:
        refs[count][...] = total.astype(BF)
        return
    size = stage[2]
    own_ref, *sent_refs, pieces_ref = refs[count:]
    rows = total.shape[0] // size
    for j in range(size):
        pieces_ref[j] = total[j * rows : (j + 1) * rows]
    hand_out(stage, pieces_ref, own_ref, sent_refs)


def sum_up(own, parts, stage):
    columns = own.shape[1]
    if stage is None:
        outs, scratch = [shape(own.shape, BF)], []
    else:
        rows = own.shape[0] // stage[2]
        outs = [shape((rows, columns))] + [shape((rows, columns), BF)] * (stage[2] - 1)
        scratch = [pltpu.VMEM((stage[2], rows, columns), F32)]
    kernel = functools.partial(sum_kernel, stage, 1 + len(parts))
    return call(kernel, outs, (own, *parts), math.prod(own.shape) * 4, scratch)


def send(stage, pieces):
    axis, stride, size = stage
    return [swap(p, axis, k * stride) for k, p in zip(order(size), pieces)]


def place_kernel(stage, own_ref, *refs):
    place = place_on(stage)
    out_ref = refs[-1]
    out_ref[place] = own_ref[...]
    for k, ref in zip(order(stage[2]), refs[:-1]):
        out_ref[lax.bitwise_xor(place, k)] = ref[...]


def scatter_start(own, sent):
    core, plane, _ = stages()
    return sum_up(own, send(core, [sent]), plane)


def scatter_rest(own, *sent):
    _, plane, line = stages()
    own, *sent = sum_up(own, send(plane, sent), line)
    return sum_up(own, send(line, sent), None)[0]


def gather(value):
    core, plane, line = stages()
    for stage in (line, plane):
        got = send(stage, [value] * (stage[2] - 1))
        rows, columns = value.shape
        kernel = functools.partial(place_kernel, stage)
        (value,) = call(
            kernel, [shape((stage[2], rows, columns), BF)], (value, *got), rows * columns
        )
        value = value.reshape(stage[2] * rows, columns)
    return value, send(core, [value])[0]


def call(kernel, outs, args, flops, scratch=()):
    spec = pl.BlockSpec(memory_space=pltpu.VMEM)
    size = sum(math.prod(o.shape) * o.dtype.itemsize for o in outs)
    size += sum(math.prod(a.shape) * a.dtype.itemsize for a in args)
    return pl.pallas_call(
        kernel,
        out_shape=outs,
        in_specs=[spec] * len(args),
        out_specs=[spec] * len(outs),
        scratch_shapes=list(scratch),
        cost_estimate=pl.CostEstimate(flops=flops, bytes_accessed=size, transcendentals=0),
        compiler_params=pltpu.CompilerParams(vmem_limit_bytes=30 * 1024 * 1024),
    )(*args)


def shape(dims, dtype=F32):
    return jax.ShapeDtypeStruct(tuple(dims), dtype)


def spans(total, step):
    count = max(total // step, 1)
    return [(n * step, total if n == count - 1 else (n + 1) * step) for n in range(count)]


def pack_kernel(field_ref, out_ref):
    rows, width, channels = field_ref.shape
    lanes = out_ref.shape[1]
    cells = rows * width
    for r in range(rows):
        out_ref[r * width : (r + 1) * width, :] = field_ref[r, :, :lanes]
    last = jnp.concatenate(
        [
            jnp.broadcast_to(field_ref[r, :, lanes:channels], (width, 128))
            for r in range(rows)
        ]
    )
    out_ref[cells : cells + 8, :] = jnp.zeros((8, lanes), F32)
    out_ref[cells : cells + 8, :cells] = last.T[:8]


def forward_kernel(
    field_ref, above_ref, below_ref, kernel_ref, gain_ref, up_ref, down_ref, head_ref,
    truth_ref, weight_in_ref, forecast_ref, miss_ref, weight_ref, win_ref, normed_ref, inverse_ref, scaled_ref, turned_ref, hidden_ref,
    slope_ref, rounded_ref, summed_ref,
):
    height, width, channels = field_ref.shape
    lanes = above_ref.shape[1]
    cells = height * width

    def put(row, main, last):
        for columns, value in ((slice(0, lanes), main), (slice(lanes, channels), last)):
            win_ref[row, 8 : 8 + width, columns] = value
            win_ref[row, 6:8, columns] = value[width - 2 :]
            win_ref[row, 8 + width : 10 + width, columns] = value[:2]

    for base, ref in ((0, above_ref), (2 + height, below_ref)):
        turned = ref[2 * width : 2 * width + 8, :].T
        for r in range(2):
            put(
                base + r,
                ref[r * width : (r + 1) * width, :],
                turned[r * width : (r + 1) * width, :1],
            )
    for r in range(height):
        put(2 + r, field_ref[r, :, :lanes], field_ref[r, :, lanes:])

    part = width // 2

    def convolve(columns):
        for half in range(2):
            first = half * part
            acc = [win_ref[i + 2, 8 + first : 8 + first + part, columns] for i in range(height)]
            for w in range(height + 4):
                for b in range(5):
                    moved = win_ref[w, 6 + b + first : 6 + b + first + part, columns]
                    for i in range(height):
                        if 0 <= w - i < 5:
                            t = 5 * (w - i) + b
                            acc[i] = acc[i] + kernel_ref[t : t + 1, columns] * moved
            for i in range(height):
                start = i * width + first
                summed_ref[start : start + part, columns] = acc[i]

    @pl.loop(0, lanes // 128)
    def _(n):
        convolve(pl.ds(pl.multiple_of(n * 128, 128), 128))

    convolve(slice(lanes, channels))

    for start in range(0, cells, part):
        rows = slice(start, start + part)
        summed = summed_ref[rows, :]
        center = summed - jnp.sum(summed, axis=1, keepdims=True) * (1.0 / channels)
        variance = jnp.sum(center * center, axis=1, keepdims=True) * (1.0 / channels)
        inverse = lax.rsqrt(variance + EPSILON)
        normed = center * inverse
        normed_ref[rows, :] = normed
        inverse_ref[rows, :] = inverse
        scaled_ref[rows, :] = (normed * gain_ref[...]).astype(BF)

    turned_ref[...] = scaled_ref[...].T
    output = summed_ref[...]
    for lo, hi in spans(up_ref.shape[1], 256):
        preact = dot(scaled_ref[...], up_ref[:, lo:hi], ((1,), (0,)))
        cumul = 0.5 * (1.0 + lax.erf(preact * (1.0 / math.sqrt(2.0))))
        density = jnp.exp(-0.5 * preact * preact) * (1.0 / math.sqrt(2.0 * math.pi))
        hidden = (preact * cumul).astype(BF)
        hidden_ref[:, lo:hi] = hidden
        slope_ref[:, lo:hi] = cumul + preact * density
        summed_ref[...] += dot(hidden, down_ref[:, lo:hi], ((1,), (1,)))
    rounded = summed_ref[...].astype(BF)
    rounded_ref[...] = rounded
    forecast = dot(head_ref[...], rounded, ((1,), (1,)))
    forecast_ref[...] = forecast
    miss_ref[...] = forecast - truth_ref[...]
    weight_ref[...] = weight_in_ref[...]


def score_kernel(members, bands, count, *refs):
    other_refs = refs[: members - 1]
    (
        forecast_ref, miss_ref, weight_ref, head_ref, down_ref, rounded_ref, hidden_ref, slope_ref,
        turned_ref, own_ref, sent_ref, output_ref, preact_ref, head_term_ref, factor_ref, loss_ref,
        cot_ref, main_ref,
    ) = refs[members - 1 :]
    fields, cells = forecast_ref.shape
    lanes = own_ref.shape[1]
    mine = lax.axis_index("mem") * bands + lax.axis_index("lat")
    forecast = forecast_ref[...]
    weights = weight_ref[...]
    miss = miss_ref[...]
    pair_abs = jnp.zeros_like(forecast)
    pair_der = jnp.zeros_like(forecast)
    for ref in other_refs:
        diff = forecast - ref[...]
        square = diff * diff + DELTA * DELTA
        inverse = lax.rsqrt(square)
        pair_abs = pair_abs + (square * inverse - DELTA)
        pair_der = pair_der + diff * inverse
    square = miss * miss + DELTA * DELTA
    inverse = lax.rsqrt(square)
    spread = (square * inverse - DELTA) * (1.0 / members) - pair_abs * (
        1.0 / (2.0 * members * (members - 1))
    )
    part = jnp.sum(jnp.sum(weights * spread, axis=1, keepdims=True), axis=0, keepdims=True)
    first = part.astype(BF).astype(F32)
    second = (part - first).astype(BF).astype(F32)
    third = part - first - second
    slot = lax.broadcasted_iota(jnp.int32, (8, lanes), 1) == mine
    line = lax.broadcasted_iota(jnp.int32, (8, lanes), 0)
    value = jnp.where(line == 0, first, jnp.where(line == 1, second, third))
    loss_ref[...] = jnp.where(slot & (line < 3), value, 0.0)
    cot = (
        weights
        * (miss * inverse - pair_der * (1.0 / (members - 1)))
        * (1.0 / (members * math.sqrt(count)))
    )
    co = cot.astype(BF)
    cot_ref[...] = jnp.zeros_like(cot_ref)
    cot_ref[:fields, :cells] = co.astype(F32)
    turned = cot_ref[...].T[:cells, :fields].astype(BF)
    head_term_ref[...] = dot(co, rounded_ref[...], ((1,), (0,)))
    d_output = dot(turned, head_ref[...], ((1,), (0,)))
    output_ref[...] = d_output
    d_round = d_output.astype(BF)
    for lo, hi in spans(down_ref.shape[1], 256):
        factor_ref[:, lo:hi] = dot(co, hidden_ref[:, lo:hi], ((1,), (0,)))
        d_hidden = dot(d_round, down_ref[:, lo:hi], ((1,), (0,)))
        preact_ref[:, lo:hi] = (d_hidden * slope_ref[:, lo:hi]).astype(BF)
    gradient_rows(main_ref, 0, main_ref.shape[0] * main_ref.shape[1], turned_ref, preact_ref)
    hand_out(stages()[0], main_ref, own_ref, [sent_ref])


def gradient_rows(out_ref, first, count, turned_ref, preact_ref):
    piece, lanes = out_ref.shape[1:]
    done = 0
    while done < count:
        h, r = (first + done) // lanes, (first + done) % lanes
        p, at = done // piece, done % piece
        take = min(lanes - r, piece - at, count - done)
        out_ref[p, at : at + take, :] = dot(
            turned_ref[r : r + take, :], preact_ref[:, h * lanes : (h + 1) * lanes], ((1,), (0,))
        )
        done += take


def rest_kernel(
    preact_ref, turned_ref, scaled_ref, up_ref, gain_ref, normed_ref, inverse_ref, output_ref,
    win_ref, head_term_ref, factor_ref, loss_ref, after_ref,
    own_ref, sent_ref, wide_ref, grads_ref, heads_ref, pieces_ref,
):
    cells, channels = normed_ref.shape
    hidden_units = preact_ref.shape[1]
    fields = head_term_ref.shape[0]
    size, piece, lanes = pieces_ref.shape
    halves = hidden_units // lanes
    even = halves * lanes
    height = win_ref.shape[0] - 4
    width = cells // height
    base = size * piece - 256
    gradient_rows(pieces_ref, halves * lanes - base, base, turned_ref, preact_ref)
    out_ref = pieces_ref.at[size - 1]
    base -= (size - 1) * piece
    for h in range(halves):
        at = base + h * fields
        out_ref[at : at + fields, :] = factor_ref[:, h * lanes : (h + 1) * lanes]
    at = base + halves * fields
    out_ref[at : at + fields, :] = head_term_ref[:, :lanes]
    at += fields

    d_scaled = dot(preact_ref[...], up_ref[...], ((1,), (1,)))
    normed = normed_ref[...]
    grads_ref[...] = jnp.zeros_like(grads_ref)
    grads_ref[25:26, :channels] = jnp.sum(d_scaled * normed, axis=0, keepdims=True)
    d_normed = d_scaled * gain_ref[...]
    d_summed = output_ref[...] + inverse_ref[...] * (
        d_normed
        - jnp.sum(d_normed, axis=1, keepdims=True) * (1.0 / channels)
        - normed * (jnp.sum(d_normed * normed, axis=1, keepdims=True) * (1.0 / channels))
    )
    wide_ref[...] = d_summed

    def correlate(columns):
        for a in range(5):
            for b in range(5):
                total = None
                for i in range(height):
                    term = jnp.sum(
                        wide_ref[i * width : (i + 1) * width, columns]
                        * win_ref[i + a, 6 + b : 6 + b + width, columns],
                        axis=0,
                        keepdims=True,
                    )
                    total = term if total is None else total + term
                t = 5 * a + b
                grads_ref[t : t + 1, columns] = total

    @pl.loop(0, lanes // 128)
    def _(n):
        correlate(pl.ds(pl.multiple_of(n * 128, 128), 128))

    correlate(slice(lanes, channels))

    out_ref[at : at + 26, :] = grads_ref[:26, :lanes]
    at += 26
    last = dot(turned_ref[lanes - 7 : channels, :], preact_ref[...], ((1,), (0,)))[7:8]
    for h in range(halves):
        out_ref[at + h : at + h + 1, :] = last[:, h * lanes : (h + 1) * lanes]
    at += halves
    left = hidden_units - even
    columns = dot(preact_ref[:, even:], scaled_ref[...], ((0,), (0,)))
    out_ref[at : at + left, :] = columns[:, :lanes]
    at += left
    out_ref[at:, :] = jnp.zeros((out_ref.shape[0] - at, lanes), F32)
    heads_ref[...] = jnp.zeros_like(heads_ref)
    heads_ref[:fields, :left] = factor_ref[:, even:]
    out_ref[at : at + left, :128] = heads_ref[...].T[:left]
    at += left
    heads_ref[:fields, :1] = head_term_ref[:, lanes:]
    out_ref[at : at + 1, :128] = heads_ref[...].T[:1]
    at += 1
    out_ref[at : at + 1, :128] = grads_ref[:, lanes : lanes + 128].T[:1]
    at += 1
    out_ref[at : at + 1, :left] = last[:, even:]
    at += 1
    out_ref[at : at + 3, :] = loss_ref[:3]
    hand_out(stages()[0], pieces_ref, own_ref, [sent_ref])


def finish_kernel(
    count, own_one_ref, got_one_ref, own_two_ref, got_two_ref, head_ref,
    loss_ref, kernel_ref, gain_ref, up_ref, down_ref, head_out_ref, one_ref, two_ref,
):
    half = own_one_ref.shape[0]
    core = place_on(stages()[0])
    for out, own, got in (
        (one_ref, own_one_ref, got_one_ref), (two_ref, own_two_ref, got_two_ref)
    ):
        out[pl.ds(pl.multiple_of(core * half, half), half), :] = own[...].astype(F32)
        out[pl.ds(pl.multiple_of((1 - core) * half, half), half), :] = got[...].astype(F32)
    channels, hidden_units = up_ref.shape
    lanes = one_ref.shape[1]
    fields = head_ref.shape[1]
    taps = kernel_ref.shape[0]
    halves = hidden_units // lanes
    even = halves * lanes
    left = hidden_units - even
    base = two_ref.shape[0] - 256
    rows = 0
    for ref, total in ((one_ref, one_ref.shape[0]), (two_ref, base)):
        at = 0
        while at < total:
            h, r = rows // lanes, rows % lanes
            take = min(lanes - r, total - at)
            up_ref[r : r + take, h * lanes : (h + 1) * lanes] = ref[at : at + take, :]
            rows += take
            at += take
    for h in range(halves):
        down_ref[:, h * lanes : (h + 1) * lanes] = dot(
            head_ref[...],
            two_ref[base + h * fields : base + (h + 1) * fields, :].astype(BF),
            ((1,), (0,)),
        )
    extra = two_ref[base:, :]
    at = halves * fields
    head_out_ref[:, :lanes] = extra[at : at + fields]
    at += fields
    kernel_ref[:, :lanes] = extra[at : at + taps]
    at += taps
    gain_ref[:, :lanes] = extra[at : at + 1]
    at += 1
    for h in range(halves):
        up_ref[lanes:channels, h * lanes : (h + 1) * lanes] = extra[at + h : at + h + 1]
    at += halves
    tail = extra[240:256].T
    up_ref[:lanes, even:] = tail[:lanes, at - 240 : at - 240 + left]
    at += left
    down_ref[:, even:] = dot(
        head_ref[...], extra[at : at + left, :fields].astype(BF), ((1,), (1,))
    )
    at += left
    head_out_ref[:, lanes:] = tail[:fields, at - 240 : at - 239]
    at += 1
    kernel_ref[:, lanes:] = tail[:taps, at - 240 : at - 239]
    gain_ref[:, lanes:] = extra[at : at + 1, taps : taps + 1]
    at += 1
    up_ref[lanes:channels, even:] = extra[at : at + 1, :left]
    at += 1
    total = extra[at : at + 1] + extra[at + 1 : at + 2] + extra[at + 2 : at + 3]
    loss_ref[...] = jnp.sum(total, axis=1, keepdims=True) * (1.0 / count)


def local(
    state, conv_kernel, norm_gain, up_weight, down_weight, field_head_weight, target, field_weight
):
    members = lax.axis_size("mem")
    bands = lax.axis_size("lat")
    field = jnp.transpose(state[0], (1, 2, 0))
    height, width, channels = field.shape
    cells = height * width
    hidden_units = up_weight.shape[1]
    nlat = bands * height
    nfields = target.shape[0]
    lanes = channels // 128 * 128
    halves = hidden_units // lanes
    down_turned = down_weight.T
    head_turned = field_head_weight.T
    gain = norm_gain[None]

    def halo(first, pairs):
        sent = call(
            pack_kernel, [shape((2 * width + 8, lanes))], (field[first : first + 2],), 1000000
        )[0]
        return lax.ppermute(sent, "lat", pairs)

    above = halo(height - 2, [(i, i + 1) for i in range(bands - 1)])
    below = halo(0, [(i + 1, i) for i in range(bands - 1)])
    row = (lax.axis_index("lat") * height + jnp.arange(height)).astype(F32)
    area = jnp.repeat(jnp.cos(0.5 * math.pi * ((row + 0.5) / nlat - 1.0)), width)
    weights = field_weight[:, None] * area[None, :]
    count = nlat * width * nfields
    truth = target.reshape(nfields, cells)

    mlp = 2 * cells * channels * hidden_units
    forecast, miss, weights, window, normed, inverse, scaled, turned, hidden, slope, rounded = call(
        forward_kernel,
        [
            shape((nfields, cells)),
            shape((nfields, cells)),
            shape((nfields, cells)),
            shape((height + 4, width + 16, channels)),
            shape((cells, channels)),
            shape((cells, 1)),
            shape((cells, channels), BF),
            shape((channels, cells), BF),
            shape((cells, hidden_units), BF),
            shape((cells, hidden_units)),
            shape((cells, channels), BF),
        ],
        (
            field, above, below, conv_kernel, gain, up_weight, down_turned, head_turned, truth,
            weights,
        ),
        2 * mlp,
        [pltpu.VMEM((cells, channels), F32)],
    )
    near = [forecast] + [swap(forecast, "mem", 2 * k) for k in order(members // 2)]
    others = near[1:] + [swap(piece, "mem", 1) for piece in near]
    main_rows = halves * lanes
    half = (main_rows + 256) // 4
    own, sent, d_output, d_preact, head_term, factor, loss_rows = call(
        functools.partial(score_kernel, members, bands, count),
        [
            shape((half, lanes)),
            shape((half, lanes)),
            shape((cells, channels)),
            shape((cells, hidden_units), BF),
            shape((nfields, channels)),
            shape((nfields, hidden_units)),
            shape((8, lanes)),
        ],
        (
            *others, forecast, miss, weights, head_turned, down_turned, rounded, hidden, slope,
            turned,
        ),
        2 * mlp,
        [
            pltpu.VMEM((128, -(-cells // 128) * 128), F32),
            pltpu.VMEM((2, half, lanes), F32),
        ],
    )
    one = scatter_start(own, sent)
    own, sent = call(
        rest_kernel,
        [shape((half, lanes)), shape((half, lanes))],
        (
            d_preact, turned, scaled, up_weight, gain, normed, inverse, d_output, window,
            head_term, factor, loss_rows, one[0],
        ),
        2 * mlp,
        [
            pltpu.VMEM((cells, channels), F32),
            pltpu.VMEM((128, lanes + 128), F32),
            pltpu.VMEM((128, 128), F32),
            pltpu.VMEM((2, half, lanes), F32),
        ],
    )
    two = scatter_start(own, sent)
    one = scatter_rest(*one)
    two = scatter_rest(*two)
    one = gather(one)
    two = gather(two)
    loss, grad_kernel, grad_gain, grad_up, grad_down, grad_head = call(
        functools.partial(finish_kernel, count),
        [
            shape((1, 1)),
            shape(conv_kernel.shape),
            shape((1, channels)),
            shape(up_weight.shape),
            shape((channels, hidden_units)),
            shape((nfields, channels)),
        ],
        (*one, *two, field_head_weight),
        mlp // 4,
        [pltpu.VMEM((2 * half, lanes), F32)] * 2,
    )
    return (
        loss.reshape(()), grad_kernel, grad_gain[0], grad_up, grad_down.T, grad_head.T,
    )


def solution(mesh):
    return jax.shard_map(
        local,
        mesh=mesh,
        in_specs=(P("mem", None, "lat", None), P(), P(), P(), P(), P(), P(None, "lat", None), P()),
        out_specs=(P(), P(), P(), P(), P(), P()),
        check_vma=False,
    )
```

```python
import functools
import math

import jax
import jax.numpy as jnp
from jax import lax
from jax.experimental import pallas as pl
from jax.experimental.pallas import tpu as pltpu
from jax.sharding import PartitionSpec as P


DELTA = 0.1
EPSILON = 1e-05
BF = jnp.bfloat16
F32 = jnp.float32


def dot(left, right, dims):
    return lax.dot_general(left, right, (dims, ((), ())), preferred_element_type=F32)


def swap(value, axis, mask):
    count = lax.axis_size(axis)
    return lax.ppermute(value, axis, [(i, i ^ mask) for i in range(count)])


def stages():
    members = lax.axis_size("mem")
    return (("mem", 1, 2), ("mem", 2, members // 2), ("lat", 1, lax.axis_size("lat")))


def order(size):
    return sorted(range(1, size), key=lambda k: -bin(k).count("1"))


def place_on(stage):
    axis, stride, size = stage
    return (lax.axis_index(axis) // stride) % size


def hand_out(stage, pieces_ref, own_ref, sent_refs):
    place = place_on(stage)
    own_ref[...] = pieces_ref[place]
    for k, ref in zip(order(stage[2]), sent_refs):
        ref[...] = pieces_ref[lax.bitwise_xor(place, k)].astype(ref.dtype)


def sum_kernel(stage, counts, *refs):
    totals = []
    for count in counts:
        total = refs[0][...]
        for ref in refs[1:count]:
            total = total + ref[...].astype(F32)
        totals.append(total)
        refs = refs[count:]
    if stage is None:
        refs[0][...] = totals[0].astype(BF)
        return
    size = stage[2]
    own_ref, *sent_refs, pieces_ref = refs
    rows = totals[0].shape[0] // size
    for n, total in enumerate(totals):
        for j in range(size):
            pieces_ref[j, n * rows : (n + 1) * rows] = total[j * rows : (j + 1) * rows]
    hand_out(stage, pieces_ref, own_ref, sent_refs)


def sum_up(groups, stage):
    length, columns = groups[0][0].shape
    if stage is None:
        outs, scratch = [shape((length, columns), BF)], []
    else:
        rows = length // stage[2] * len(groups)
        outs = [shape((rows, columns))] + [shape((rows, columns), BF)] * (stage[2] - 1)
        scratch = [pltpu.VMEM((stage[2], rows, columns), F32)]
    kernel = functools.partial(sum_kernel, stage, [len(g) for g in groups])
    return call(kernel, outs, sum(groups, ()), length * columns * 4, scratch)


def send(stage, pieces):
    axis, stride, size = stage
    return [swap(p, axis, k * stride) for k, p in zip(order(size), pieces)]


def place_kernel(stage, own_ref, *refs):
    place = place_on(stage)
    out_ref = refs[-1]
    out_ref[place] = own_ref[...]
    for k, ref in zip(order(stage[2]), refs[:-1]):
        out_ref[lax.bitwise_xor(place, k)] = ref[...]


def collect(value, got, stage):
    rows, columns = value.shape
    kernel = functools.partial(place_kernel, stage)
    (out,) = call(kernel, [shape((stage[2], rows, columns), BF)], (value, *got), rows * columns)
    return out.reshape(stage[2] * rows, columns)


def scatter_start(own, sent):
    core, plane, _ = stages()
    return sum_up([(own, *send(core, [sent]))], plane)


def across_plane(own, *sent):
    return (own, *send(stages()[1], sent))


def finish_exchange(group):
    core, plane, line = stages()
    own, *sent = sum_up([group], line)
    got = send(line, sent)
    value = sum_up([(own, *got)], None)[0]
    for stage in (line, plane):
        got = send(stage, [value] * (stage[2] - 1))
        value = collect(value, got, stage)
    return value, send(core, [value])[0]


def call(kernel, outs, args, flops, scratch=()):
    spec = pl.BlockSpec(memory_space=pltpu.VMEM)
    size = sum(math.prod(o.shape) * o.dtype.itemsize for o in outs)
    size += sum(math.prod(a.shape) * a.dtype.itemsize for a in args)
    return pl.pallas_call(
        kernel,
        out_shape=outs,
        in_specs=[spec] * len(args),
        out_specs=[spec] * len(outs),
        scratch_shapes=list(scratch),
        cost_estimate=pl.CostEstimate(flops=flops, bytes_accessed=size, transcendentals=0),
        compiler_params=pltpu.CompilerParams(vmem_limit_bytes=30 * 1024 * 1024),
    )(*args)


def shape(dims, dtype=F32):
    return jax.ShapeDtypeStruct(tuple(dims), dtype)


def spans(total, step):
    count = max(total // step, 1)
    return [(n * step, total if n == count - 1 else (n + 1) * step) for n in range(count)]


def pack_kernel(field_ref, out_ref):
    rows, width, channels = field_ref.shape
    lanes = out_ref.shape[1]
    cells = rows * width
    for r in range(rows):
        out_ref[r * width : (r + 1) * width, :] = field_ref[r, :, :lanes]
    last = jnp.concatenate(
        [
            jnp.broadcast_to(field_ref[r, :, lanes:channels], (width, 128))
            for r in range(rows)
        ]
    )
    out_ref[cells : cells + 8, :] = jnp.zeros((8, lanes), F32)
    out_ref[cells : cells + 8, :cells] = last.T[:8]


def fill(win_ref, row, main, last):
    width = main.shape[0]
    lanes = main.shape[1]
    channels = win_ref.shape[2]
    for columns, value in ((slice(0, lanes), main), (slice(lanes, channels), last)):
        win_ref[row, 8 : 8 + width, columns] = value
        win_ref[row, 6:8, columns] = value[width - 2 :]
        win_ref[row, 8 + width : 10 + width, columns] = value[:2]


def convolve(win_ref, kernel_ref, rows, sum_in_ref, sum_ref, first_row, height, width):
    lanes = kernel_ref.shape[1] // 128 * 128
    part = width // 2

    def block(columns):
        for half in range(2):
            first = half * part
            spans = [slice(i * width + first, i * width + first + part) for i in range(height)]
            acc = [
                win_ref[i + 2 - first_row, 8 + first : 8 + first + part, columns]
                if sum_in_ref is None
                else sum_in_ref[spans[i], columns]
                for i in range(height)
            ]
            for w in rows:
                for b in range(5):
                    at = 6 + b + first
                    moved = win_ref[w - first_row, at : at + part, columns]
                    for i in range(height):
                        if 0 <= w - i < 5:
                            t = 5 * (w - i) + b
                            acc[i] = acc[i] + kernel_ref[t : t + 1, columns] * moved
            for i in range(height):
                sum_ref[spans[i], columns] = acc[i]

    @pl.loop(0, lanes // 128)
    def _(n):
        block(pl.ds(pl.multiple_of(n * 128, 128), 128))

    block(slice(lanes, kernel_ref.shape[1]))


def prep_kernel(
    bands, field_ref, kernel_ref, gain_in_ref, target_ref, field_weight_ref, early_up_ref,
    early_head_ref, part_ref, gain_ref, truth_ref, weight_ref, win_ref, turn_ref,
):
    height, width, channels = field_ref.shape
    lanes = channels // 128 * 128
    fields, _ = truth_ref.shape
    for r in range(height):
        fill(win_ref, r, field_ref[r, :, :lanes], field_ref[r, :, lanes:])
    convolve(win_ref, kernel_ref, range(2, 2 + height), None, part_ref, 2, height, width)
    gain_ref[...] = gain_in_ref[...][None, :]
    turn_ref[...] = jnp.zeros_like(turn_ref)
    turn_ref[:1, :fields] = field_weight_ref[...][None, :]
    column = turn_ref[...].T[:fields, :1]
    base = (lax.axis_index("lat") * height).astype(F32)
    for r in range(height):
        truth_ref[:, r * width : (r + 1) * width] = target_ref[:, r, :]
        row = jnp.full((1, width), r, F32) + base
        area = jnp.cos(0.5 * math.pi * ((row + 0.5) / (bands * height) - 1.0))
        weight_ref[:, r * width : (r + 1) * width] = column * area


def forward_kernel(
    field_ref, part_ref, first_ref, second_ref, kernel_ref, gain_ref, up_ref, down_ref, head_ref,
    truth_ref, forecast_ref, miss_ref, win_ref, normed_ref, inverse_ref, scaled_ref, turned_ref, hidden_ref,
    slope_ref, rounded_ref, summed_ref,
):
    height, width, channels = field_ref.shape
    lanes = first_ref.shape[1]
    cells = height * width

    odd = lax.axis_index("lat") % 2 == 1
    for base, odds_ref, evens_ref in (
        (0, first_ref, second_ref), (2 + height, second_ref, first_ref)
    ):
        rows = jnp.where(odd, odds_ref[...], evens_ref[...])
        turned = rows[2 * width : 2 * width + 8, :].T
        for r in range(2):
            span = slice(r * width, (r + 1) * width)
            fill(win_ref, base + r, rows[span, :], turned[span, :1])
    for r in range(height):
        fill(win_ref, 2 + r, field_ref[r, :, :lanes], field_ref[r, :, lanes:])
    rows = [w for w in range(height + 4) if not 2 <= w < 2 + height]
    convolve(win_ref, kernel_ref, rows, part_ref, summed_ref, 0, height, width)
    part = width // 2
    for start in range(0, cells, part):
        rows = slice(start, start + part)
        summed = summed_ref[rows, :]
        center = summed - jnp.sum(summed, axis=1, keepdims=True) * (1.0 / channels)
        variance = jnp.sum(center * center, axis=1, keepdims=True) * (1.0 / channels)
        inverse = lax.rsqrt(variance + EPSILON)
        normed = center * inverse
        normed_ref[rows, :] = normed
        inverse_ref[rows, :] = inverse
        scaled_ref[rows, :] = (normed * gain_ref[...]).astype(BF)

    turned_ref[...] = scaled_ref[...].T
    for lo, hi in spans(up_ref.shape[1], 256):
        preact = dot(scaled_ref[...], up_ref[:, lo:hi], ((1,), (0,)))
        cumul = 0.5 * (1.0 + lax.erf(preact * (1.0 / math.sqrt(2.0))))
        density = jnp.exp(-0.5 * preact * preact) * (1.0 / math.sqrt(2.0 * math.pi))
        hidden = (preact * cumul).astype(BF)
        hidden_ref[:, lo:hi] = hidden
        slope_ref[:, lo:hi] = cumul + preact * density
        summed_ref[...] += dot(hidden, down_ref[:, lo:hi], ((1,), (1,)))
    rounded = summed_ref[...].astype(BF)
    rounded_ref[...] = rounded
    forecast = dot(head_ref[...], rounded, ((1,), (1,)))
    forecast_ref[...] = forecast
    miss_ref[...] = forecast - truth_ref[...]


def score_kernel(members, bands, count, *refs):
    other_refs = refs[: members - 1]
    (
        forecast_ref, miss_ref, weight_ref, head_ref, down_ref, rounded_ref, hidden_ref, slope_ref,
        turned_ref, own_ref, sent_ref, output_ref, preact_ref, head_term_ref, factor_ref, loss_ref,
        cot_ref, main_ref,
    ) = refs[members - 1 :]
    fields, cells = forecast_ref.shape
    lanes = own_ref.shape[1]
    mine = lax.axis_index("mem") * bands + lax.axis_index("lat")
    forecast = forecast_ref[...]
    weights = weight_ref[...]
    miss = miss_ref[...]
    pair_abs = jnp.zeros_like(forecast)
    pair_der = jnp.zeros_like(forecast)
    for ref in other_refs:
        diff = forecast - ref[...]
        square = diff * diff + DELTA * DELTA
        inverse = lax.rsqrt(square)
        pair_abs = pair_abs + (square * inverse - DELTA)
        pair_der = pair_der + diff * inverse
    square = miss * miss + DELTA * DELTA
    inverse = lax.rsqrt(square)
    spread = (square * inverse - DELTA) * (1.0 / members) - pair_abs * (
        1.0 / (2.0 * members * (members - 1))
    )
    part = jnp.sum(jnp.sum(weights * spread, axis=1, keepdims=True), axis=0, keepdims=True)
    first = part.astype(BF).astype(F32)
    second = (part - first).astype(BF).astype(F32)
    third = part - first - second
    slot = lax.broadcasted_iota(jnp.int32, (8, lanes), 1) == mine
    line = lax.broadcasted_iota(jnp.int32, (8, lanes), 0)
    value = jnp.where(line == 0, first, jnp.where(line == 1, second, third))
    loss_ref[...] = jnp.where(slot & (line < 3), value, 0.0)
    cot = (
        weights
        * (miss * inverse - pair_der * (1.0 / (members - 1)))
        * (1.0 / (members * math.sqrt(count)))
    )
    co = cot.astype(BF)
    cot_ref[...] = jnp.zeros_like(cot_ref)
    cot_ref[:fields, :cells] = co.astype(F32)
    turned = cot_ref[...].T[:cells, :fields].astype(BF)
    head_term_ref[...] = dot(co, rounded_ref[...], ((1,), (0,)))
    d_output = dot(turned, head_ref[...], ((1,), (0,)))
    output_ref[...] = d_output
    d_round = d_output.astype(BF)
    for lo, hi in spans(down_ref.shape[1], 256):
        factor_ref[:, lo:hi] = dot(co, hidden_ref[:, lo:hi], ((1,), (0,)))
        d_hidden = dot(d_round, down_ref[:, lo:hi], ((1,), (0,)))
        preact_ref[:, lo:hi] = (d_hidden * slope_ref[:, lo:hi]).astype(BF)
    gradient_rows(main_ref, 0, main_ref.shape[0] * main_ref.shape[1], turned_ref, preact_ref)
    hand_out(stages()[0], main_ref, own_ref, [sent_ref])


def gradient_rows(out_ref, first, count, turned_ref, preact_ref):
    piece, lanes = out_ref.shape[1:]
    done = 0
    while done < count:
        h, r = (first + done) // lanes, (first + done) % lanes
        p, at = done // piece, done % piece
        take = min(lanes - r, piece - at, count - done)
        out_ref[p, at : at + take, :] = dot(
            turned_ref[r : r + take, :], preact_ref[:, h * lanes : (h + 1) * lanes], ((1,), (0,))
        )
        done += take


def rest_kernel(
    preact_ref, turned_ref, scaled_ref, up_ref, gain_ref, normed_ref, inverse_ref, output_ref,
    win_ref, head_term_ref, factor_ref, loss_ref, after_ref,
    own_ref, sent_ref, wide_ref, grads_ref, heads_ref, pieces_ref,
):
    cells, channels = normed_ref.shape
    hidden_units = preact_ref.shape[1]
    fields = head_term_ref.shape[0]
    size, piece, lanes = pieces_ref.shape
    halves = hidden_units // lanes
    even = halves * lanes
    height = win_ref.shape[0] - 4
    width = cells // height
    base = size * piece - 256
    gradient_rows(pieces_ref, halves * lanes - base, base, turned_ref, preact_ref)
    out_ref = pieces_ref.at[size - 1]
    base -= (size - 1) * piece
    for h in range(halves):
        at = base + h * fields
        out_ref[at : at + fields, :] = factor_ref[:, h * lanes : (h + 1) * lanes]
    at = base + halves * fields
    out_ref[at : at + fields, :] = head_term_ref[:, :lanes]
    at += fields

    d_scaled = dot(preact_ref[...], up_ref[...], ((1,), (1,)))
    normed = normed_ref[...]
    grads_ref[...] = jnp.zeros_like(grads_ref)
    grads_ref[25:26, :channels] = jnp.sum(d_scaled * normed, axis=0, keepdims=True)
    d_normed = d_scaled * gain_ref[...]
    d_summed = output_ref[...] + inverse_ref[...] * (
        d_normed
        - jnp.sum(d_normed, axis=1, keepdims=True) * (1.0 / channels)
        - normed * (jnp.sum(d_normed * normed, axis=1, keepdims=True) * (1.0 / channels))
    )
    wide_ref[...] = d_summed

    def correlate(columns):
        for a in range(5):
            for b in range(5):
                total = None
                for i in range(height):
                    term = jnp.sum(
                        wide_ref[i * width : (i + 1) * width, columns]
                        * win_ref[i + a, 6 + b : 6 + b + width, columns],
                        axis=0,
                        keepdims=True,
                    )
                    total = term if total is None else total + term
                t = 5 * a + b
                grads_ref[t : t + 1, columns] = total

    @pl.loop(0, lanes // 128)
    def _(n):
        correlate(pl.ds(pl.multiple_of(n * 128, 128), 128))

    correlate(slice(lanes, channels))

    out_ref[at : at + 26, :] = grads_ref[:26, :lanes]
    at += 26
    last = dot(turned_ref[lanes - 7 : channels, :], preact_ref[...], ((1,), (0,)))[7:8]
    for h in range(halves):
        out_ref[at + h : at + h + 1, :] = last[:, h * lanes : (h + 1) * lanes]
    at += halves
    left = hidden_units - even
    columns = dot(preact_ref[:, even:], scaled_ref[...], ((0,), (0,)))
    out_ref[at : at + left, :] = columns[:, :lanes]
    at += left
    out_ref[at:, :] = jnp.zeros((out_ref.shape[0] - at, lanes), F32)
    heads_ref[...] = jnp.zeros_like(heads_ref)
    heads_ref[:fields, :left] = factor_ref[:, even:]
    out_ref[at : at + left, :128] = heads_ref[...].T[:left]
    at += left
    heads_ref[:fields, :1] = head_term_ref[:, lanes:]
    out_ref[at : at + 1, :128] = heads_ref[...].T[:1]
    at += 1
    out_ref[at : at + 1, :128] = grads_ref[:, lanes : lanes + 128].T[:1]
    at += 1
    out_ref[at : at + 1, :left] = last[:, even:]
    at += 1
    out_ref[at : at + 3, :] = loss_ref[:3]
    hand_out(stages()[0], pieces_ref, own_ref, [sent_ref])


def finish_kernel(
    count, own_one_ref, got_one_ref, own_two_ref, got_two_ref, head_ref,
    loss_ref, kernel_ref, gain_ref, up_ref, down_ref, head_out_ref, one_ref, two_ref,
):
    core = place_on(stages()[0])
    for out, own, got in (
        (one_ref, own_one_ref, got_one_ref), (two_ref, own_two_ref, got_two_ref)
    ):
        out[core] = own[...].astype(F32)
        out[1 - core] = got[...].astype(F32)
    channels, hidden_units = up_ref.shape
    lanes = one_ref.shape[2]
    fields = head_ref.shape[1]
    taps = kernel_ref.shape[0]
    halves = hidden_units // lanes
    even = halves * lanes
    left = hidden_units - even
    rows = 0
    for ref in (one_ref.at[0], one_ref.at[1], two_ref.at[0], two_ref.at[1]):
        at = 0
        while at < ref.shape[0] and rows < even:
            h, r = rows // lanes, rows % lanes
            take = min(lanes - r, ref.shape[0] - at, even - rows)
            up_ref[r : r + take, h * lanes : (h + 1) * lanes] = ref[at : at + take, :]
            rows += take
            at += take
    extra = two_ref.at[1][two_ref.shape[1] - 256 :, :]
    for h in range(halves):
        down_ref[:, h * lanes : (h + 1) * lanes] = dot(
            head_ref[...], extra[h * fields : (h + 1) * fields, :].astype(BF), ((1,), (0,))
        )
    at = halves * fields
    head_out_ref[:, :lanes] = extra[at : at + fields]
    at += fields
    kernel_ref[:, :lanes] = extra[at : at + taps]
    at += taps
    gain_ref[:, :lanes] = extra[at : at + 1]
    at += 1
    for h in range(halves):
        up_ref[lanes:channels, h * lanes : (h + 1) * lanes] = extra[at + h : at + h + 1]
    at += halves
    tail = extra[240:256].T
    up_ref[:lanes, even:] = tail[:lanes, at - 240 : at - 240 + left]
    at += left
    down_ref[:, even:] = dot(
        head_ref[...], extra[at : at + left, :fields].astype(BF), ((1,), (1,))
    )
    at += left
    head_out_ref[:, lanes:] = tail[:fields, at - 240 : at - 239]
    at += 1
    kernel_ref[:, lanes:] = tail[:taps, at - 240 : at - 239]
    gain_ref[:, lanes:] = extra[at : at + 1, taps : taps + 1]
    at += 1
    up_ref[lanes:channels, even:] = extra[at : at + 1, :left]
    at += 1
    total = extra[at : at + 1] + extra[at + 1 : at + 2] + extra[at + 2 : at + 3]
    loss_ref[...] = jnp.sum(total, axis=1, keepdims=True) * (1.0 / count)


def local(
    state, conv_kernel, norm_gain, up_weight, down_weight, field_head_weight, target, field_weight
):
    members = lax.axis_size("mem")
    bands = lax.axis_size("lat")
    field = jnp.transpose(state[0], (1, 2, 0))
    height, width, channels = field.shape
    cells = height * width
    hidden_units = up_weight.shape[1]
    nlat = bands * height
    nfields = target.shape[0]
    lanes = channels // 128 * 128
    halves = hidden_units // lanes
    down_turned = down_weight.T
    head_turned = field_head_weight.T

    odd = lax.axis_index("lat") % 2

    def packed(first):
        return call(
            pack_kernel, [shape((2 * width + 8, lanes))], (field[first : first + 2],), 1000000
        )[0]

    def trade(value, start):
        pairs = [(i, i + 1) for i in range(start, bands - 1, 2)]
        return lax.ppermute(value, "lat", pairs + [(j, i) for i, j in pairs])

    head = packed(0)
    tail = head if height == 2 else packed(height - 2)
    if height == 2:
        traded = [trade(head, 0), trade(head, 1)]
    else:
        traded = [
            trade(jnp.where(odd == 0, tail, head), 0), trade(jnp.where(odd == 0, head, tail), 1)
        ]
    count = nlat * width * nfields
    part, gain, truth, weights = call(
        functools.partial(prep_kernel, bands),
        [
            shape((cells, channels)),
            shape((1, channels)),
            shape((nfields, cells)),
            shape((nfields, cells)),
        ],
        (field, conv_kernel, norm_gain, target, field_weight, up_weight, head_turned),
        10**8,
        [pltpu.VMEM((height, width + 16, channels), F32), pltpu.VMEM((128, 128), F32)],
    )
    mlp = 2 * cells * channels * hidden_units
    forecast, miss, window, normed, inverse, scaled, turned, hidden, slope, rounded = call(
        forward_kernel,
        [
            shape((nfields, cells)),
            shape((nfields, cells)),
            shape((height + 4, width + 16, channels)),
            shape((cells, channels)),
            shape((cells, 1)),
            shape((cells, channels), BF),
            shape((channels, cells), BF),
            shape((cells, hidden_units), BF),
            shape((cells, hidden_units)),
            shape((cells, channels), BF),
        ],
        (
            field, part, *traded, conv_kernel, gain, up_weight, down_turned, head_turned,
            truth,
        ),
        2 * mlp,
        [pltpu.VMEM((cells, channels), F32)],
    )
    near = [forecast] + [swap(forecast, "mem", 2 * k) for k in order(members // 2)]
    others = near[1:] + [swap(piece, "mem", 1) for piece in near]
    main_rows = halves * lanes
    half = (main_rows + 256) // 4
    small_half = half
    own, sent, d_output, d_preact, head_term, factor, loss_rows = call(
        functools.partial(score_kernel, members, bands, count),
        [
            shape((half, lanes)),
            shape((half, lanes)),
            shape((cells, channels)),
            shape((cells, hidden_units), BF),
            shape((nfields, channels)),
            shape((nfields, hidden_units)),
            shape((8, lanes)),
        ],
        (
            *others, forecast, miss, weights, head_turned, down_turned, rounded, hidden, slope,
            turned,
        ),
        2 * mlp,
        [
            pltpu.VMEM((128, -(-cells // 128) * 128), F32),
            pltpu.VMEM((2, half, lanes), F32),
        ],
    )
    one = scatter_start(own, sent)
    first = across_plane(*one)
    own, sent = call(
        rest_kernel,
        [shape((small_half, lanes)), shape((small_half, lanes))],
        (
            d_preact, turned, scaled, up_weight, gain, normed, inverse, d_output, window,
            head_term, factor, loss_rows, one[0],
        ),
        2 * mlp,
        [
            pltpu.VMEM((cells, channels), F32),
            pltpu.VMEM((128, lanes + 128), F32),
            pltpu.VMEM((128, 128), F32),
            pltpu.VMEM((2, small_half, lanes), F32),
        ],
    )
    two = scatter_start(own, sent)
    second = across_plane(*two)
    one = finish_exchange(first)
    two = finish_exchange(second)
    loss, grad_kernel, grad_gain, grad_up, grad_down, grad_head = call(
        functools.partial(finish_kernel, count),
        [
            shape((1, 1)),
            shape(conv_kernel.shape),
            shape((1, channels)),
            shape(up_weight.shape),
            shape((channels, hidden_units)),
            shape((nfields, channels)),
        ],
        (*one, *two, field_head_weight),
        mlp // 4,
        [pltpu.VMEM((2, half, lanes), F32), pltpu.VMEM((2, small_half, lanes), F32)],
    )
    return (
        loss.reshape(()), grad_kernel, grad_gain[0], grad_up, grad_down.T, grad_head.T,
    )


def solution(mesh):
    return jax.shard_map(
        local,
        mesh=mesh,
        in_specs=(P("mem", None, "lat", None), P(), P(), P(), P(), P(), P(None, "lat", None), P()),
        out_specs=(P(), P(), P(), P(), P(), P()),
        check_vma=False,
    )
```

```python
import functools
import math

import jax
import jax.numpy as jnp
from jax import lax
from jax.experimental import pallas as pl
from jax.experimental.pallas import tpu as pltpu
from jax.sharding import PartitionSpec as P


DELTA = 0.1
EPSILON = 1e-05
BF = jnp.bfloat16
EXTRA = (224, 32)
F32 = jnp.float32


def dot(left, right, dims):
    return lax.dot_general(left, right, (dims, ((), ())), preferred_element_type=F32)


def swap(value, axis, mask):
    count = lax.axis_size(axis)
    return lax.ppermute(value, axis, [(i, i ^ mask) for i in range(count)])


def stages():
    members = lax.axis_size("mem")
    return (("mem", 1, 2), ("mem", 2, members // 2), ("lat", 1, lax.axis_size("lat")))


def order(size):
    return sorted(range(1, size), key=lambda k: -bin(k).count("1"))


def place_on(stage):
    axis, stride, size = stage
    return (lax.axis_index(axis) // stride) % size


def hand_out(stage, pieces_ref, own_ref, sent_refs):
    place = place_on(stage)
    own_ref[...] = pieces_ref[place]
    for k, ref in zip(order(stage[2]), sent_refs):
        ref[...] = pieces_ref[lax.bitwise_xor(place, k)].astype(ref.dtype)


def sum_kernel(stage, counts, *refs):
    totals = []
    for count in counts:
        total = refs[0][...]
        for ref in refs[1:count]:
            total = total + ref[...].astype(F32)
        totals.append(total)
        refs = refs[count:]
    if stage is None:
        refs[0][...] = totals[0].astype(BF)
        return
    size = stage[2]
    own_ref, *sent_refs, pieces_ref = refs
    rows = totals[0].shape[0] // size
    for n, total in enumerate(totals):
        for j in range(size):
            pieces_ref[j, n * rows : (n + 1) * rows] = total[j * rows : (j + 1) * rows]
    hand_out(stage, pieces_ref, own_ref, sent_refs)


def sum_up(groups, stage):
    length, columns = groups[0][0].shape
    if stage is None:
        outs, scratch = [shape((length, columns), BF)], []
    else:
        rows = length // stage[2] * len(groups)
        outs = [shape((rows, columns))] + [shape((rows, columns), BF)] * (stage[2] - 1)
        scratch = [pltpu.VMEM((stage[2], rows, columns), F32)]
    kernel = functools.partial(sum_kernel, stage, [len(g) for g in groups])
    return call(kernel, outs, sum(groups, ()), length * columns * 4, scratch)


def send(stage, pieces):
    axis, stride, size = stage
    return [swap(p, axis, k * stride) for k, p in zip(order(size), pieces)]


def place_kernel(stage, own_ref, *refs):
    place = place_on(stage)
    out_ref = refs[-1]
    out_ref[place] = own_ref[...]
    for k, ref in zip(order(stage[2]), refs[:-1]):
        out_ref[lax.bitwise_xor(place, k)] = ref[...]


def collect(value, got, stage):
    rows, columns = value.shape
    kernel = functools.partial(place_kernel, stage)
    (out,) = call(kernel, [shape((stage[2], rows, columns), BF)], (value, *got), rows * columns)
    return out.reshape(stage[2] * rows, columns)


def scatter_start(own, sent):
    core, plane, _ = stages()
    return sum_up([(own, *send(core, [sent]))], plane)


def across_plane(own, *sent):
    return (own, *send(stages()[1], sent))


def finish_exchange(group):
    core, plane, line = stages()
    own, *sent = sum_up([group], line)
    got = send(line, sent)
    value = sum_up([(own, *got)], None)[0]
    for stage in (line, plane):
        got = send(stage, [value] * (stage[2] - 1))
        value = collect(value, got, stage)
    return value, send(core, [value])[0]


def call(kernel, outs, args, flops, scratch=()):
    spec = pl.BlockSpec(memory_space=pltpu.VMEM)
    size = sum(math.prod(o.shape) * o.dtype.itemsize for o in outs)
    size += sum(math.prod(a.shape) * a.dtype.itemsize for a in args)
    return pl.pallas_call(
        kernel,
        out_shape=outs,
        in_specs=[spec] * len(args),
        out_specs=[spec] * len(outs),
        scratch_shapes=list(scratch),
        cost_estimate=pl.CostEstimate(flops=flops, bytes_accessed=size, transcendentals=0),
        compiler_params=pltpu.CompilerParams(vmem_limit_bytes=30 * 1024 * 1024),
    )(*args)


def shape(dims, dtype=F32):
    return jax.ShapeDtypeStruct(tuple(dims), dtype)


def spans(total, step):
    count = max(total // step, 1)
    return [(n * step, total if n == count - 1 else (n + 1) * step) for n in range(count)]


def pack_kernel(field_ref, out_ref):
    rows, width, channels = field_ref.shape
    lanes = out_ref.shape[1]
    cells = rows * width
    for r in range(rows):
        out_ref[r * width : (r + 1) * width, :] = field_ref[r, :, :lanes]
    last = jnp.concatenate(
        [
            jnp.broadcast_to(field_ref[r, :, lanes:channels], (width, 128))
            for r in range(rows)
        ]
    )
    out_ref[cells : cells + 8, :] = jnp.zeros((8, lanes), F32)
    out_ref[cells : cells + 8, :cells] = last.T[:8]


def fill(win_ref, row, main, last):
    width = main.shape[0]
    lanes = main.shape[1]
    channels = win_ref.shape[2]
    for columns, value in ((slice(0, lanes), main), (slice(lanes, channels), last)):
        win_ref[row, 8 : 8 + width, columns] = value
        win_ref[row, 6:8, columns] = value[width - 2 :]
        win_ref[row, 8 + width : 10 + width, columns] = value[:2]


def convolve(win_ref, kernel_ref, rows, sum_in_ref, sum_ref, first_row, height, width):
    lanes = kernel_ref.shape[1] // 128 * 128
    part = width // 2

    def block(columns):
        for half in range(2):
            first = half * part
            spans = [slice(i * width + first, i * width + first + part) for i in range(height)]
            acc = [
                win_ref[i + 2 - first_row, 8 + first : 8 + first + part, columns]
                if sum_in_ref is None
                else sum_in_ref[spans[i], columns]
                for i in range(height)
            ]
            for w in rows:
                for b in range(5):
                    at = 6 + b + first
                    moved = win_ref[w - first_row, at : at + part, columns]
                    for i in range(height):
                        if 0 <= w - i < 5:
                            t = 5 * (w - i) + b
                            acc[i] = acc[i] + kernel_ref[t : t + 1, columns] * moved
            for i in range(height):
                sum_ref[spans[i], columns] = acc[i]

    @pl.loop(0, lanes // 128)
    def _(n):
        block(pl.ds(pl.multiple_of(n * 128, 128), 128))

    block(slice(lanes, kernel_ref.shape[1]))


def prep_kernel(
    bands, field_ref, kernel_ref, gain_in_ref, target_ref, field_weight_ref, early_up_ref,
    early_head_ref, part_ref, gain_ref, truth_ref, weight_ref, win_ref, turn_ref,
):
    height, width, channels = field_ref.shape
    lanes = channels // 128 * 128
    fields, _ = truth_ref.shape
    for r in range(height):
        fill(win_ref, r, field_ref[r, :, :lanes], field_ref[r, :, lanes:])
    convolve(win_ref, kernel_ref, range(2, 2 + height), None, part_ref, 2, height, width)
    gain_ref[...] = gain_in_ref[...][None, :]
    turn_ref[...] = jnp.zeros_like(turn_ref)
    turn_ref[:1, :fields] = field_weight_ref[...][None, :]
    column = turn_ref[...].T[:fields, :1]
    base = (lax.axis_index("lat") * height).astype(F32)
    for r in range(height):
        truth_ref[:, r * width : (r + 1) * width] = target_ref[:, r, :]
        row = jnp.full((1, width), r, F32) + base
        area = jnp.cos(0.5 * math.pi * ((row + 0.5) / (bands * height) - 1.0))
        weight_ref[:, r * width : (r + 1) * width] = column * area


def forward_kernel(
    field_ref, part_ref, first_ref, second_ref, kernel_ref, gain_ref, up_ref, down_ref, head_ref,
    truth_ref, forecast_ref, miss_ref, win_ref, normed_ref, inverse_ref, scaled_ref, hidden_ref,
    preact_ref, rounded_ref, summed_ref,
):
    height, width, channels = field_ref.shape
    lanes = first_ref.shape[1]
    cells = height * width

    odd = lax.axis_index("lat") % 2 == 1
    for base, odds_ref, evens_ref in (
        (0, first_ref, second_ref), (2 + height, second_ref, first_ref)
    ):
        rows = jnp.where(odd, odds_ref[...], evens_ref[...])
        turned = rows[2 * width : 2 * width + 8, :].T
        for r in range(2):
            span = slice(r * width, (r + 1) * width)
            fill(win_ref, base + r, rows[span, :], turned[span, :1])
    for r in range(height):
        fill(win_ref, 2 + r, field_ref[r, :, :lanes], field_ref[r, :, lanes:])
    rows = [w for w in range(height + 4) if not 2 <= w < 2 + height]
    convolve(win_ref, kernel_ref, rows, part_ref, summed_ref, 0, height, width)
    part = width // 2
    for start in range(0, cells, part):
        rows = slice(start, start + part)
        summed = summed_ref[rows, :]
        center = summed - jnp.sum(summed, axis=1, keepdims=True) * (1.0 / channels)
        variance = jnp.sum(center * center, axis=1, keepdims=True) * (1.0 / channels)
        inverse = lax.rsqrt(variance + EPSILON)
        normed = center * inverse
        normed_ref[rows, :] = normed
        inverse_ref[rows, :] = inverse
        scaled_ref[rows, :] = (normed * gain_ref[...]).astype(BF)

    for lo, hi in spans(up_ref.shape[1], 256):
        preact = dot(scaled_ref[...], up_ref[:, lo:hi], ((1,), (0,)))
        preact_ref[:, lo:hi] = preact
        cumul = 0.5 * (1.0 + lax.erf(preact * (1.0 / math.sqrt(2.0))))
        hidden = (preact * cumul).astype(BF)
        hidden_ref[:, lo:hi] = hidden
        summed_ref[...] += dot(hidden, down_ref[:, lo:hi], ((1,), (1,)))
    rounded = summed_ref[...].astype(BF)
    rounded_ref[...] = rounded
    forecast = dot(head_ref[...], rounded, ((1,), (1,)))
    forecast_ref[...] = forecast
    miss_ref[...] = forecast - truth_ref[...]


def slope_kernel(preact_ref, scaled_ref, slope_ref, turned_ref):
    turned_ref[...] = scaled_ref[...].T
    for lo, hi in spans(preact_ref.shape[1], 256):
        preact = preact_ref[:, lo:hi]
        cumul = 0.5 * (1.0 + lax.erf(preact * (1.0 / math.sqrt(2.0))))
        density = jnp.exp(-0.5 * preact * preact) * (1.0 / math.sqrt(2.0 * math.pi))
        slope_ref[:, lo:hi] = cumul + preact * density


def score_kernel(members, bands, count, *refs):
    other_refs = refs[: members - 1]
    (
        forecast_ref, miss_ref, weight_ref, head_ref, down_ref, rounded_ref, hidden_ref, slope_ref,
        turned_ref, own_ref, sent_ref, output_ref, preact_ref,
        cot_ref, main_ref, factor_ref, heads_ref,
    ) = refs[members - 1 :]
    fields, cells = forecast_ref.shape
    lanes = own_ref.shape[1]
    mine = lax.axis_index("mem") * bands + lax.axis_index("lat")
    forecast = forecast_ref[...]
    weights = weight_ref[...]
    miss = miss_ref[...]
    pair_abs = jnp.zeros_like(forecast)
    pair_der = jnp.zeros_like(forecast)
    for ref in other_refs:
        diff = forecast - ref[...]
        square = diff * diff + DELTA * DELTA
        inverse = lax.rsqrt(square)
        pair_abs = pair_abs + (square * inverse - DELTA)
        pair_der = pair_der + diff * inverse
    square = miss * miss + DELTA * DELTA
    inverse = lax.rsqrt(square)
    spread = (square * inverse - DELTA) * (1.0 / members) - pair_abs * (
        1.0 / (2.0 * members * (members - 1))
    )
    part = jnp.sum(jnp.sum(weights * spread, axis=1, keepdims=True), axis=0, keepdims=True)
    first = part.astype(BF).astype(F32)
    second = (part - first).astype(BF).astype(F32)
    third = part - first - second
    slot = lax.broadcasted_iota(jnp.int32, (1, lanes), 1) == mine
    losses = [jnp.where(slot, value, 0.0) for value in (first, second, third)]
    cot = (
        weights
        * (miss * inverse - pair_der * (1.0 / (members - 1)))
        * (1.0 / (members * math.sqrt(count)))
    )
    co = cot.astype(BF)
    cot_ref[...] = jnp.zeros_like(cot_ref)
    cot_ref[:fields, :cells] = co.astype(F32)
    turned = cot_ref[...].T[:cells, :fields].astype(BF)
    head_term = dot(co, rounded_ref[...], ((1,), (0,)))
    d_output = dot(turned, head_ref[...], ((1,), (0,)))
    output_ref[...] = d_output
    d_round = d_output.astype(BF)
    for lo, hi in spans(down_ref.shape[1], 256):
        factor_ref[:, lo:hi] = dot(co, hidden_ref[:, lo:hi], ((1,), (0,)))
        d_hidden = dot(d_round, down_ref[:, lo:hi], ((1,), (0,)))
        preact_ref[:, lo:hi] = (d_hidden * slope_ref[:, lo:hi]).astype(BF)
    size, piece, lanes = main_ref.shape
    gradient_rows(main_ref, 0, size * piece - EXTRA[0], turned_ref, preact_ref)
    out_ref = main_ref.at[size - 1]
    halves = down_ref.shape[1] // lanes
    even = halves * lanes
    left = down_ref.shape[1] - even
    at = piece - EXTRA[0]
    for h in range(halves):
        out_ref[at : at + fields, :] = factor_ref[:, h * lanes : (h + 1) * lanes]
        at += fields
    out_ref[at : at + fields, :] = head_term[:, :lanes]
    at += fields
    out_ref[at:, :] = jnp.zeros((piece - at, lanes), F32)
    heads_ref[...] = jnp.zeros_like(heads_ref)
    heads_ref[:fields, :left] = factor_ref[:, even:]
    heads_ref[:fields, left : left + 1] = head_term[:, lanes:]
    out_ref[at : at + left + 1, :128] = heads_ref[...].T[: left + 1]
    at += left + 1
    for n, value in enumerate(losses):
        out_ref[at + n : at + n + 1, :] = value
    hand_out(stages()[0], main_ref, own_ref, [sent_ref])


def gradient_rows(out_ref, first, count, turned_ref, preact_ref):
    piece, lanes = out_ref.shape[1:]
    done = 0
    while done < count:
        h, r = (first + done) // lanes, (first + done) % lanes
        p, at = done // piece, done % piece
        take = min(lanes - r, piece - at, count - done)
        out_ref[p, at : at + take, :] = dot(
            turned_ref[r : r + take, :], preact_ref[:, h * lanes : (h + 1) * lanes], ((1,), (0,))
        )
        done += take


def input_kernel(
    preact_ref, up_ref, gain_ref, normed_ref, inverse_ref, output_ref, wide_ref, gain_row_ref
):
    channels = normed_ref.shape[1]
    d_scaled = dot(preact_ref[...], up_ref[...], ((1,), (1,)))
    normed = normed_ref[...]
    gain_row_ref[...] = jnp.sum(d_scaled * normed, axis=0, keepdims=True)
    d_normed = d_scaled * gain_ref[...]
    d_summed = output_ref[...] + inverse_ref[...] * (
        d_normed
        - jnp.sum(d_normed, axis=1, keepdims=True) * (1.0 / channels)
        - normed * (jnp.sum(d_normed * normed, axis=1, keepdims=True) * (1.0 / channels))
    )
    wide_ref[...] = d_summed


def rest_kernel(
    preact_ref, turned_ref, scaled_ref, win_ref, wide_ref, gain_row_ref, after_ref,
    own_ref, sent_ref, grads_ref, pieces_ref,
):
    cells, channels = wide_ref.shape
    hidden_units = preact_ref.shape[1]
    size, piece, lanes = pieces_ref.shape
    halves = hidden_units // lanes
    even = halves * lanes
    height = win_ref.shape[0] - 4
    width = cells // height
    base = size * piece - EXTRA[1]
    gradient_rows(pieces_ref, even - base, base, turned_ref, preact_ref)
    out_ref = pieces_ref.at[size - 1]
    at = piece - EXTRA[1]

    grads_ref[...] = jnp.zeros_like(grads_ref)
    grads_ref[25:26, :channels] = gain_row_ref[...]
    part = width // 4

    def correlate(columns):
        acc = [None] * 25
        for c in range(0, width, part):
            d = [wide_ref[i * width + c : i * width + c + part, columns] for i in range(height)]
            for w in range(height + 4):
                for b in range(5):
                    moved = win_ref[w, 6 + b + c : 6 + b + c + part, columns]
                    for i in range(height):
                        if 0 <= w - i < 5:
                            t = 5 * (w - i) + b
                            term = d[i] * moved
                            for r in range(0, part, 8):
                                value = term[r : r + 8]
                                acc[t] = value if acc[t] is None else acc[t] + value
        for t in range(25):
            grads_ref[t : t + 1, columns] = jnp.sum(acc[t], axis=0, keepdims=True)

    @pl.loop(0, lanes // 128)
    def _(n):
        correlate(pl.ds(pl.multiple_of(n * 128, 128), 128))

    correlate(slice(lanes, channels))

    out_ref[at : at + 26, :] = grads_ref[:26, :lanes]
    at += 26
    last = dot(turned_ref[lanes - 7 : channels, :], preact_ref[...], ((1,), (0,)))[7:8]
    for h in range(halves):
        out_ref[at + h : at + h + 1, :] = last[:, h * lanes : (h + 1) * lanes]
    at += halves
    left = hidden_units - even
    columns = dot(preact_ref[:, even:], scaled_ref[...], ((0,), (0,)))
    out_ref[at : at + left, :] = columns[:, :lanes]
    at += left
    out_ref[at:, :] = jnp.zeros((out_ref.shape[0] - at, lanes), F32)
    out_ref[at : at + 1, :128] = grads_ref[:, lanes : lanes + 128].T[:1]
    at += 1
    out_ref[at : at + 1, :left] = last[:, even:]
    hand_out(stages()[0], pieces_ref, own_ref, [sent_ref])


def finish_down_kernel(count, own_ref, got_ref, head_ref, loss_ref, down_ref, head_out_ref):
    lanes = own_ref.shape[1]
    fields = head_ref.shape[1]
    hidden_units = down_ref.shape[1]
    halves = hidden_units // lanes
    even = halves * lanes
    left = hidden_units - even
    span = slice(own_ref.shape[0] - EXTRA[0], own_ref.shape[0])
    mine = place_on(stages()[0]) == 1
    extra = jnp.where(mine, own_ref[span, :].astype(F32), got_ref[span, :].astype(F32))
    factor = extra.astype(BF)
    for h in range(halves):
        down_ref[:, h * lanes : (h + 1) * lanes] = dot(
            head_ref[...], factor[h * fields : (h + 1) * fields], ((1,), (0,))
        )
    at = halves * fields
    head_out_ref[:, :lanes] = extra[at : at + fields]
    at += fields
    down_ref[:, even:] = dot(head_ref[...], factor[at : at + left, :fields], ((1,), (1,)))
    tail = extra[at : at + 8].T
    head_out_ref[:, lanes:] = tail[:fields, left : left + 1]
    at += left + 1
    total = extra[at : at + 1] + extra[at + 1 : at + 2] + extra[at + 2 : at + 3]
    loss_ref[...] = jnp.sum(total, axis=1, keepdims=True) * (1.0 / count)


def finish_up_kernel(
    own_one_ref, got_one_ref, own_two_ref, got_two_ref,
    kernel_ref, gain_ref, up_ref, one_ref, two_ref,
):
    core = place_on(stages()[0])
    for out, own, got in (
        (one_ref, own_one_ref, got_one_ref), (two_ref, own_two_ref, got_two_ref)
    ):
        out[core] = own[...].astype(F32)
        out[1 - core] = got[...].astype(F32)
    channels, hidden_units = up_ref.shape
    size, piece, lanes = one_ref.shape
    taps = kernel_ref.shape[0]
    halves = hidden_units // lanes
    even = halves * lanes
    left = hidden_units - even
    rows = 0
    for chunk, ref in enumerate((one_ref, two_ref)):
        for p in range(size):
            at = 0
            end = piece - (EXTRA[chunk] if p == size - 1 else 0)
            while at < end:
                h, r = rows // lanes, rows % lanes
                take = min(lanes - r, end - at)
                up_ref[r : r + take, h * lanes : (h + 1) * lanes] = ref[p, at : at + take, :]
                rows += take
                at += take
    extra = two_ref[size - 1, piece - EXTRA[1] :, :]
    tail = extra.T
    kernel_ref[:, :lanes] = extra[:taps]
    at = taps
    gain_main = extra[at]
    at += 1
    for h in range(halves):
        up_ref[lanes:channels, h * lanes : (h + 1) * lanes] = extra[at + h : at + h + 1]
    at += halves
    up_ref[:lanes, even:] = tail[:lanes, at : at + left]
    at += left
    kernel_ref[:, lanes:] = tail[:taps, at : at + 1]
    gain_ref[:lanes] = gain_main
    gain_ref[lanes:] = extra[at, taps : taps + 1]
    at += 1
    up_ref[lanes:channels, even:] = extra[at : at + 1, :left]


def local(
    state, conv_kernel, norm_gain, up_weight, down_weight, field_head_weight, target, field_weight
):
    members = lax.axis_size("mem")
    bands = lax.axis_size("lat")
    field = jnp.transpose(state[0], (1, 2, 0))
    height, width, channels = field.shape
    cells = height * width
    hidden_units = up_weight.shape[1]
    nlat = bands * height
    nfields = target.shape[0]
    lanes = channels // 128 * 128
    halves = hidden_units // lanes
    down_turned = down_weight.T
    head_turned = field_head_weight.T

    odd = lax.axis_index("lat") % 2

    def packed(first):
        return call(
            pack_kernel, [shape((2 * width + 8, lanes))], (field[first : first + 2],), 1000000
        )[0]

    def trade(value, start):
        pairs = [(i, i + 1) for i in range(start, bands - 1, 2)]
        return lax.ppermute(value, "lat", pairs + [(j, i) for i, j in pairs])

    head = packed(0)
    tail = head if height == 2 else packed(height - 2)
    if height == 2:
        traded = [trade(head, 0), trade(head, 1)]
    else:
        traded = [
            trade(jnp.where(odd == 0, tail, head), 0), trade(jnp.where(odd == 0, head, tail), 1)
        ]
    count = nlat * width * nfields
    part, gain, truth, weights = call(
        functools.partial(prep_kernel, bands),
        [
            shape((cells, channels)),
            shape((1, channels)),
            shape((nfields, cells)),
            shape((nfields, cells)),
        ],
        (field, conv_kernel, norm_gain, target, field_weight, up_weight, head_turned),
        10**8,
        [pltpu.VMEM((height, width + 16, channels), F32), pltpu.VMEM((128, 128), F32)],
    )
    mlp = 2 * cells * channels * hidden_units
    forecast, miss, window, normed, inverse, scaled, hidden, preact, rounded = call(
        forward_kernel,
        [
            shape((nfields, cells)),
            shape((nfields, cells)),
            shape((height + 4, width + 16, channels)),
            shape((cells, channels)),
            shape((cells, 1)),
            shape((cells, channels), BF),
            shape((cells, hidden_units), BF),
            shape((cells, hidden_units)),
            shape((cells, channels), BF),
        ],
        (
            field, part, *traded, conv_kernel, gain, up_weight, down_turned, head_turned,
            truth,
        ),
        2 * mlp,
        [pltpu.VMEM((cells, channels), F32)],
    )
    near = [forecast] + [swap(forecast, "mem", 2 * k) for k in order(members // 2)]
    slope, turned = call(
        slope_kernel,
        [shape((cells, hidden_units)), shape((channels, cells), BF)],
        (preact, scaled),
        mlp,
    )
    others = near[1:] + [swap(piece, "mem", 1) for piece in near]
    main_rows = halves * lanes
    half = (main_rows + sum(EXTRA)) // 4
    own, sent, d_output, d_preact = call(
        functools.partial(score_kernel, members, bands, count),
        [
            shape((half, lanes)),
            shape((half, lanes)),
            shape((cells, channels)),
            shape((cells, hidden_units), BF),
        ],
        (
            *others, forecast, miss, weights, head_turned, down_turned, rounded, hidden, slope,
            turned,
        ),
        2 * mlp,
        [
            pltpu.VMEM((128, -(-cells // 128) * 128), F32),
            pltpu.VMEM((2, half, lanes), F32),
            pltpu.VMEM((nfields, hidden_units), F32),
            pltpu.VMEM((128, 128), F32),
        ],
    )
    got = send(stages()[0], [sent])
    wide, gain_row = call(
        input_kernel,
        [shape((cells, channels)), shape((1, channels))],
        (d_preact, up_weight, gain, normed, inverse, d_output),
        mlp,
    )
    one = sum_up([(own, *got)], stages()[1])
    first = across_plane(*one)
    own, sent = call(
        rest_kernel,
        [shape((half, lanes)), shape((half, lanes))],
        (
            d_preact, turned, scaled, window, wide, gain_row,
            one[0],
        ),
        2 * mlp,
        [
            pltpu.VMEM((128, lanes + 128), F32),
            pltpu.VMEM((2, half, lanes), F32),
        ],
    )
    two = scatter_start(own, sent)
    second = across_plane(*two)
    one = finish_exchange(first)
    two = finish_exchange(second)
    loss, grad_down, grad_head = call(
        functools.partial(finish_down_kernel, count),
        [shape((1, 1)), shape((channels, hidden_units)), shape((nfields, channels))],
        (*one, field_head_weight),
        mlp // 4,
    )
    grad_kernel, grad_gain, grad_up = call(
        finish_up_kernel,
        [shape(conv_kernel.shape), shape((channels,)), shape(up_weight.shape)],
        (*one, *two),
        mlp // 4,
        [pltpu.VMEM((2, half, lanes), F32)] * 2,
    )
    return (
        loss.reshape(()), grad_kernel, grad_gain, grad_up, grad_down.T, grad_head.T,
    )


def solution(mesh):
    return jax.shard_map(
        local,
        mesh=mesh,
        in_specs=(P("mem", None, "lat", None), P(), P(), P(), P(), P(), P(None, "lat", None), P()),
        out_specs=(P(), P(), P(), P(), P(), P()),
        check_vma=False,
    )
```

```python
import functools
import math

import jax
import jax.numpy as jnp
from jax import lax
from jax.experimental import pallas as pl
from jax.experimental.pallas import tpu as pltpu
from jax.sharding import PartitionSpec as P


DELTA = 0.1
EPSILON = 1e-05
BF = jnp.bfloat16
EXTRA = (224, 32)
F32 = jnp.float32


def dot(left, right, dims):
    return lax.dot_general(left, right, (dims, ((), ())), preferred_element_type=F32)


def swap(value, axis, mask):
    count = lax.axis_size(axis)
    return lax.ppermute(value, axis, [(i, i ^ mask) for i in range(count)])


def stages():
    members = lax.axis_size("mem")
    return (("mem", 1, 2), ("mem", 2, members // 2), ("lat", 1, lax.axis_size("lat")))


def order(size):
    return list(range(size - 1, 0, -1))


def place_on(stage):
    axis, stride, size = stage
    return (lax.axis_index(axis) // stride) % size


def hand_out(stage, pieces_ref, own_ref, sent_refs):
    place = place_on(stage)
    own_ref[...] = pieces_ref[place]
    for k, ref in zip(order(stage[2]), sent_refs):
        ref[...] = pieces_ref[lax.bitwise_xor(place, k)].astype(ref.dtype)


def sum_kernel(stage, counts, *refs):
    totals = []
    for count in counts:
        total = refs[0][...]
        for ref in refs[1:count]:
            total = total + ref[...].astype(F32)
        totals.append(total)
        refs = refs[count:]
    if stage is None:
        refs[0][...] = totals[0].astype(BF)
        return
    size = stage[2]
    own_ref, *sent_refs, pieces_ref = refs
    rows = totals[0].shape[0] // size
    for n, total in enumerate(totals):
        for j in range(size):
            pieces_ref[j, n * rows : (n + 1) * rows] = total[j * rows : (j + 1) * rows]
    hand_out(stage, pieces_ref, own_ref, sent_refs)


def sum_up(groups, stage):
    length, columns = groups[0][0].shape
    if stage is None:
        outs, scratch = [shape((length, columns), BF)], []
    else:
        rows = length // stage[2] * len(groups)
        outs = [shape((rows, columns))] + [shape((rows, columns), BF)] * (stage[2] - 1)
        scratch = [pltpu.VMEM((stage[2], rows, columns), F32)]
    kernel = functools.partial(sum_kernel, stage, [len(g) for g in groups])
    return call(kernel, outs, sum(groups, ()), length * columns * 4, scratch)


def send(stage, pieces):
    axis, stride, size = stage
    return [swap(p, axis, k * stride) for k, p in zip(order(size), pieces)]


def place_kernel(stage, own_ref, *refs):
    place = place_on(stage)
    out_ref = refs[-1]
    out_ref[place] = own_ref[...]
    for k, ref in zip(order(stage[2]), refs[:-1]):
        out_ref[lax.bitwise_xor(place, k)] = ref[...]


def collect(value, got, stage):
    rows, columns = value.shape
    kernel = functools.partial(place_kernel, stage)
    (out,) = call(kernel, [shape((stage[2], rows, columns), BF)], (value, *got), rows * columns)
    return out.reshape(stage[2] * rows, columns)


def scatter_start(own, sent):
    core, plane, _ = stages()
    return sum_up([(own, *send(core, [sent]))], plane)


def across_plane(own, *sent):
    return (own, *send(stages()[1], sent))


def finish_exchange(group):
    core, plane, line = stages()
    own, *sent = sum_up([group], line)
    got = send(line, sent)
    value = sum_up([(own, *got)], None)[0]
    for stage in (line, plane):
        got = send(stage, [value] * (stage[2] - 1))
        value = collect(value, got, stage)
    return value, send(core, [value])[0]


def call(kernel, outs, args, flops, scratch=()):
    spec = pl.BlockSpec(memory_space=pltpu.VMEM)
    size = sum(math.prod(o.shape) * o.dtype.itemsize for o in outs)
    size += sum(math.prod(a.shape) * a.dtype.itemsize for a in args)
    return pl.pallas_call(
        kernel,
        out_shape=outs,
        in_specs=[spec] * len(args),
        out_specs=[spec] * len(outs),
        scratch_shapes=list(scratch),
        cost_estimate=pl.CostEstimate(flops=flops, bytes_accessed=size, transcendentals=0),
        compiler_params=pltpu.CompilerParams(vmem_limit_bytes=30 * 1024 * 1024),
    )(*args)


def shape(dims, dtype=F32):
    return jax.ShapeDtypeStruct(tuple(dims), dtype)


def spans(total, step):
    count = max(total // step, 1)
    return [(n * step, total if n == count - 1 else (n + 1) * step) for n in range(count)]


def pack_kernel(field_ref, out_ref):
    rows, width, channels = field_ref.shape
    lanes = out_ref.shape[1]
    cells = rows * width
    for r in range(rows):
        out_ref[r * width : (r + 1) * width, :] = field_ref[r, :, :lanes]
    last = jnp.concatenate(
        [
            jnp.broadcast_to(field_ref[r, :, lanes:channels], (width, 128))
            for r in range(rows)
        ]
    )
    out_ref[cells : cells + 8, :] = jnp.zeros((8, lanes), F32)
    out_ref[cells : cells + 8, :cells] = last.T[:8]


def fill(win_ref, row, main, last):
    width = main.shape[0]
    lanes = main.shape[1]
    channels = win_ref.shape[2]
    for columns, value in ((slice(0, lanes), main), (slice(lanes, channels), last)):
        win_ref[row, 8 : 8 + width, columns] = value
        win_ref[row, 6:8, columns] = value[width - 2 :]
        win_ref[row, 8 + width : 10 + width, columns] = value[:2]


def convolve(win_ref, kernel_ref, rows, sum_in_ref, sum_ref, first_row, height, width):
    lanes = kernel_ref.shape[1] // 128 * 128
    part = width // 2

    def block(columns):
        for half in range(2):
            first = half * part
            spans = [slice(i * width + first, i * width + first + part) for i in range(height)]
            acc = [
                win_ref[i + 2 - first_row, 8 + first : 8 + first + part, columns]
                if sum_in_ref is None
                else sum_in_ref[spans[i], columns]
                for i in range(height)
            ]
            for w in rows:
                for b in range(5):
                    at = 6 + b + first
                    moved = win_ref[w - first_row, at : at + part, columns]
                    for i in range(height):
                        if 0 <= w - i < 5:
                            t = 5 * (w - i) + b
                            acc[i] = acc[i] + kernel_ref[t : t + 1, columns] * moved
            for i in range(height):
                sum_ref[spans[i], columns] = acc[i]

    @pl.loop(0, lanes // 128)
    def _(n):
        block(pl.ds(pl.multiple_of(n * 128, 128), 128))

    block(slice(lanes, kernel_ref.shape[1]))


def prep_kernel(
    bands, field_ref, kernel_ref, gain_in_ref, target_ref, field_weight_ref, early_up_ref,
    early_head_ref, part_ref, gain_ref, truth_ref, weight_ref, win_ref, turn_ref,
):
    height, width, channels = field_ref.shape
    lanes = channels // 128 * 128
    fields, _ = truth_ref.shape
    for r in range(height):
        fill(win_ref, r, field_ref[r, :, :lanes], field_ref[r, :, lanes:])
    convolve(win_ref, kernel_ref, range(2, 2 + height), None, part_ref, 2, height, width)
    gain_ref[...] = gain_in_ref[...][None, :]
    turn_ref[...] = jnp.zeros_like(turn_ref)
    turn_ref[:1, :fields] = field_weight_ref[...][None, :]
    column = turn_ref[...].T[:fields, :1]
    base = (lax.axis_index("lat") * height).astype(F32)
    for r in range(height):
        truth_ref[:, r * width : (r + 1) * width] = target_ref[:, r, :]
        row = jnp.full((1, width), r, F32) + base
        area = jnp.cos(0.5 * math.pi * ((row + 0.5) / (bands * height) - 1.0))
        weight_ref[:, r * width : (r + 1) * width] = column * area


def forward_kernel(
    field_ref, part_ref, first_ref, second_ref, kernel_ref, gain_ref, up_ref, down_ref, head_ref,
    truth_ref, forecast_ref, miss_ref, win_ref, normed_ref, inverse_ref, scaled_ref, hidden_ref,
    preact_ref, rounded_ref, summed_ref,
):
    height, width, channels = field_ref.shape
    lanes = first_ref.shape[1]
    cells = height * width

    odd = lax.axis_index("lat") % 2 == 1
    for base, odds_ref, evens_ref in (
        (0, first_ref, second_ref), (2 + height, second_ref, first_ref)
    ):
        rows = jnp.where(odd, odds_ref[...], evens_ref[...])
        turned = rows[2 * width : 2 * width + 8, :].T
        for r in range(2):
            span = slice(r * width, (r + 1) * width)
            fill(win_ref, base + r, rows[span, :], turned[span, :1])
    for r in range(height):
        fill(win_ref, 2 + r, field_ref[r, :, :lanes], field_ref[r, :, lanes:])
    rows = [w for w in range(height + 4) if not 2 <= w < 2 + height]
    convolve(win_ref, kernel_ref, rows, part_ref, summed_ref, 0, height, width)
    part = width // 2
    for start in range(0, cells, part):
        rows = slice(start, start + part)
        summed = summed_ref[rows, :]
        center = summed - jnp.sum(summed, axis=1, keepdims=True) * (1.0 / channels)
        variance = jnp.sum(center * center, axis=1, keepdims=True) * (1.0 / channels)
        inverse = lax.rsqrt(variance + EPSILON)
        normed = center * inverse
        normed_ref[rows, :] = normed
        inverse_ref[rows, :] = inverse
        scaled_ref[rows, :] = (normed * gain_ref[...]).astype(BF)

    for lo, hi in spans(up_ref.shape[1], 256):
        preact = dot(scaled_ref[...], up_ref[:, lo:hi], ((1,), (0,)))
        preact_ref[:, lo:hi] = preact
        cumul = 0.5 * (1.0 + lax.erf(preact * (1.0 / math.sqrt(2.0))))
        hidden = (preact * cumul).astype(BF)
        hidden_ref[:, lo:hi] = hidden
        summed_ref[...] += dot(hidden, down_ref[:, lo:hi], ((1,), (1,)))
    rounded = summed_ref[...].astype(BF)
    rounded_ref[...] = rounded
    forecast = dot(head_ref[...], rounded, ((1,), (1,)))
    forecast_ref[...] = forecast
    miss_ref[...] = forecast - truth_ref[...]


def slope_kernel(preact_ref, scaled_ref, slope_ref, turned_ref):
    turned_ref[...] = scaled_ref[...].T
    for lo, hi in spans(preact_ref.shape[1], 256):
        preact = preact_ref[:, lo:hi]
        cumul = 0.5 * (1.0 + lax.erf(preact * (1.0 / math.sqrt(2.0))))
        density = jnp.exp(-0.5 * preact * preact) * (1.0 / math.sqrt(2.0 * math.pi))
        slope_ref[:, lo:hi] = cumul + preact * density


def score_kernel(members, bands, count, *refs):
    other_refs = refs[: members - 1]
    (
        forecast_ref, miss_ref, weight_ref, head_ref, down_ref, rounded_ref, hidden_ref, slope_ref,
        turned_ref, own_ref, sent_ref, output_ref, preact_ref,
        cot_ref, main_ref, factor_ref, heads_ref,
    ) = refs[members - 1 :]
    fields, cells = forecast_ref.shape
    lanes = own_ref.shape[1]
    mine = lax.axis_index("mem") * bands + lax.axis_index("lat")
    forecast = forecast_ref[...]
    weights = weight_ref[...]
    miss = miss_ref[...]
    pair_abs = jnp.zeros_like(forecast)
    pair_der = jnp.zeros_like(forecast)
    for ref in other_refs:
        diff = forecast - ref[...]
        square = diff * diff + DELTA * DELTA
        inverse = lax.rsqrt(square)
        pair_abs = pair_abs + (square * inverse - DELTA)
        pair_der = pair_der + diff * inverse
    square = miss * miss + DELTA * DELTA
    inverse = lax.rsqrt(square)
    spread = (square * inverse - DELTA) * (1.0 / members) - pair_abs * (
        1.0 / (2.0 * members * (members - 1))
    )
    part = jnp.sum(jnp.sum(weights * spread, axis=1, keepdims=True), axis=0, keepdims=True)
    first = part.astype(BF).astype(F32)
    second = (part - first).astype(BF).astype(F32)
    third = part - first - second
    slot = lax.broadcasted_iota(jnp.int32, (1, lanes), 1) == mine
    losses = [jnp.where(slot, value, 0.0) for value in (first, second, third)]
    cot = (
        weights
        * (miss * inverse - pair_der * (1.0 / (members - 1)))
        * (1.0 / (members * math.sqrt(count)))
    )
    co = cot.astype(BF)
    cot_ref[...] = jnp.zeros_like(cot_ref)
    cot_ref[:fields, :cells] = co.astype(F32)
    turned = cot_ref[...].T[:cells, :fields].astype(BF)
    head_term = dot(co, rounded_ref[...], ((1,), (0,)))
    d_output = dot(turned, head_ref[...], ((1,), (0,)))
    output_ref[...] = d_output
    d_round = d_output.astype(BF)
    for lo, hi in spans(down_ref.shape[1], 256):
        factor_ref[:, lo:hi] = dot(co, hidden_ref[:, lo:hi], ((1,), (0,)))
        d_hidden = dot(d_round, down_ref[:, lo:hi], ((1,), (0,)))
        preact_ref[:, lo:hi] = (d_hidden * slope_ref[:, lo:hi]).astype(BF)
    size, piece, lanes = main_ref.shape
    gradient_rows(main_ref, 0, size * piece - EXTRA[0], turned_ref, preact_ref)
    out_ref = main_ref.at[size - 1]
    halves = down_ref.shape[1] // lanes
    even = halves * lanes
    left = down_ref.shape[1] - even
    at = piece - EXTRA[0]
    for h in range(halves):
        out_ref[at : at + fields, :] = factor_ref[:, h * lanes : (h + 1) * lanes]
        at += fields
    out_ref[at : at + fields, :] = head_term[:, :lanes]
    at += fields
    out_ref[at:, :] = jnp.zeros((piece - at, lanes), F32)
    heads_ref[...] = jnp.zeros_like(heads_ref)
    heads_ref[:fields, :left] = factor_ref[:, even:]
    heads_ref[:fields, left : left + 1] = head_term[:, lanes:]
    out_ref[at : at + left + 1, :128] = heads_ref[...].T[: left + 1]
    at += left + 1
    for n, value in enumerate(losses):
        out_ref[at + n : at + n + 1, :] = value
    hand_out(stages()[0], main_ref, own_ref, [sent_ref])


def gradient_rows(out_ref, first, count, turned_ref, preact_ref):
    piece, lanes = out_ref.shape[1:]
    done = 0
    while done < count:
        h, r = (first + done) // lanes, (first + done) % lanes
        p, at = done // piece, done % piece
        take = min(lanes - r, piece - at, count - done)
        out_ref[p, at : at + take, :] = dot(
            turned_ref[r : r + take, :], preact_ref[:, h * lanes : (h + 1) * lanes], ((1,), (0,))
        )
        done += take


def input_kernel(
    preact_ref, up_ref, gain_ref, normed_ref, inverse_ref, output_ref, wide_ref, gain_row_ref
):
    channels = normed_ref.shape[1]
    d_scaled = dot(preact_ref[...], up_ref[...], ((1,), (1,)))
    normed = normed_ref[...]
    gain_row_ref[...] = jnp.sum(d_scaled * normed, axis=0, keepdims=True)
    d_normed = d_scaled * gain_ref[...]
    d_summed = output_ref[...] + inverse_ref[...] * (
        d_normed
        - jnp.sum(d_normed, axis=1, keepdims=True) * (1.0 / channels)
        - normed * (jnp.sum(d_normed * normed, axis=1, keepdims=True) * (1.0 / channels))
    )
    wide_ref[...] = d_summed


def rest_kernel(
    preact_ref, turned_ref, scaled_ref, win_ref, wide_ref, gain_row_ref, after_ref,
    own_ref, sent_ref, grads_ref, pieces_ref,
):
    cells, channels = wide_ref.shape
    hidden_units = preact_ref.shape[1]
    size, piece, lanes = pieces_ref.shape
    halves = hidden_units // lanes
    even = halves * lanes
    height = win_ref.shape[0] - 4
    width = cells // height
    base = size * piece - EXTRA[1]
    gradient_rows(pieces_ref, even - base, base, turned_ref, preact_ref)
    out_ref = pieces_ref.at[size - 1]
    at = piece - EXTRA[1]

    grads_ref[...] = jnp.zeros_like(grads_ref)
    grads_ref[25:26, :channels] = gain_row_ref[...]
    part = width // 4

    def correlate(columns):
        acc = [None] * 25
        for c in range(0, width, part):
            d = [wide_ref[i * width + c : i * width + c + part, columns] for i in range(height)]
            for w in range(height + 4):
                for b in range(5):
                    moved = win_ref[w, 6 + b + c : 6 + b + c + part, columns]
                    for i in range(height):
                        if 0 <= w - i < 5:
                            t = 5 * (w - i) + b
                            term = d[i] * moved
                            for r in range(0, part, 8):
                                value = term[r : r + 8]
                                acc[t] = value if acc[t] is None else acc[t] + value
        for t in range(25):
            grads_ref[t : t + 1, columns] = jnp.sum(acc[t], axis=0, keepdims=True)

    @pl.loop(0, lanes // 128)
    def _(n):
        correlate(pl.ds(pl.multiple_of(n * 128, 128), 128))

    correlate(slice(lanes, channels))

    out_ref[at : at + 26, :] = grads_ref[:26, :lanes]
    at += 26
    last = dot(turned_ref[lanes - 7 : channels, :], preact_ref[...], ((1,), (0,)))[7:8]
    for h in range(halves):
        out_ref[at + h : at + h + 1, :] = last[:, h * lanes : (h + 1) * lanes]
    at += halves
    left = hidden_units - even
    columns = dot(preact_ref[:, even:], scaled_ref[...], ((0,), (0,)))
    out_ref[at : at + left, :] = columns[:, :lanes]
    at += left
    out_ref[at:, :] = jnp.zeros((out_ref.shape[0] - at, lanes), F32)
    out_ref[at : at + 1, :128] = grads_ref[:, lanes : lanes + 128].T[:1]
    at += 1
    out_ref[at : at + 1, :left] = last[:, even:]
    hand_out(stages()[0], pieces_ref, own_ref, [sent_ref])


def finish_down_kernel(count, own_ref, got_ref, head_ref, loss_ref, down_ref, head_out_ref):
    lanes = own_ref.shape[1]
    fields = head_ref.shape[1]
    hidden_units = down_ref.shape[1]
    halves = hidden_units // lanes
    even = halves * lanes
    left = hidden_units - even
    span = slice(own_ref.shape[0] - EXTRA[0], own_ref.shape[0])
    mine = place_on(stages()[0]) == 1
    extra = jnp.where(mine, own_ref[span, :].astype(F32), got_ref[span, :].astype(F32))
    factor = extra.astype(BF)
    for h in range(halves):
        down_ref[:, h * lanes : (h + 1) * lanes] = dot(
            head_ref[...], factor[h * fields : (h + 1) * fields], ((1,), (0,))
        )
    at = halves * fields
    head_out_ref[:, :lanes] = extra[at : at + fields]
    at += fields
    down_ref[:, even:] = dot(head_ref[...], factor[at : at + left, :fields], ((1,), (1,)))
    tail = extra[at : at + 8].T
    head_out_ref[:, lanes:] = tail[:fields, left : left + 1]
    at += left + 1
    total = extra[at : at + 1] + extra[at + 1 : at + 2] + extra[at + 2 : at + 3]
    loss_ref[...] = jnp.sum(total, axis=1, keepdims=True) * (1.0 / count)


def finish_up_kernel(
    own_one_ref, got_one_ref, own_two_ref, got_two_ref,
    kernel_ref, gain_ref, up_ref, one_ref, two_ref,
):
    core = place_on(stages()[0])
    for out, own, got in (
        (one_ref, own_one_ref, got_one_ref), (two_ref, own_two_ref, got_two_ref)
    ):
        out[core] = own[...].astype(F32)
        out[1 - core] = got[...].astype(F32)
    channels, hidden_units = up_ref.shape
    size, piece, lanes = one_ref.shape
    taps = kernel_ref.shape[0]
    halves = hidden_units // lanes
    even = halves * lanes
    left = hidden_units - even
    rows = 0
    for chunk, ref in enumerate((one_ref, two_ref)):
        for p in range(size):
            at = 0
            end = piece - (EXTRA[chunk] if p == size - 1 else 0)
            while at < end:
                h, r = rows // lanes, rows % lanes
                take = min(lanes - r, end - at)
                up_ref[r : r + take, h * lanes : (h + 1) * lanes] = ref[p, at : at + take, :]
                rows += take
                at += take
    extra = two_ref[size - 1, piece - EXTRA[1] :, :]
    tail = extra.T
    kernel_ref[:, :lanes] = extra[:taps]
    at = taps
    gain_main = extra[at]
    at += 1
    for h in range(halves):
        up_ref[lanes:channels, h * lanes : (h + 1) * lanes] = extra[at + h : at + h + 1]
    at += halves
    up_ref[:lanes, even:] = tail[:lanes, at : at + left]
    at += left
    kernel_ref[:, lanes:] = tail[:taps, at : at + 1]
    gain_ref[:lanes] = gain_main
    gain_ref[lanes:] = extra[at, taps : taps + 1]
    at += 1
    up_ref[lanes:channels, even:] = extra[at : at + 1, :left]


def local(
    state, conv_kernel, norm_gain, up_weight, down_weight, field_head_weight, target, field_weight
):
    members = lax.axis_size("mem")
    bands = lax.axis_size("lat")
    field = jnp.transpose(state[0], (1, 2, 0))
    height, width, channels = field.shape
    cells = height * width
    hidden_units = up_weight.shape[1]
    nlat = bands * height
    nfields = target.shape[0]
    lanes = channels // 128 * 128
    halves = hidden_units // lanes
    down_turned = down_weight.T
    head_turned = field_head_weight.T

    odd = lax.axis_index("lat") % 2

    def packed(first):
        return call(
            pack_kernel, [shape((2 * width + 8, lanes))], (field[first : first + 2],), 1000000
        )[0]

    def trade(value, start):
        pairs = [(i, i + 1) for i in range(start, bands - 1, 2)]
        return lax.ppermute(value, "lat", pairs + [(j, i) for i, j in pairs])

    head = packed(0)
    tail = head if height == 2 else packed(height - 2)
    if height == 2:
        traded = [trade(head, 0), trade(head, 1)]
    else:
        traded = [
            trade(jnp.where(odd == 0, tail, head), 0), trade(jnp.where(odd == 0, head, tail), 1)
        ]
    count = nlat * width * nfields
    part, gain, truth, weights = call(
        functools.partial(prep_kernel, bands),
        [
            shape((cells, channels)),
            shape((1, channels)),
            shape((nfields, cells)),
            shape((nfields, cells)),
        ],
        (field, conv_kernel, norm_gain, target, field_weight, up_weight, head_turned),
        10**8,
        [pltpu.VMEM((height, width + 16, channels), F32), pltpu.VMEM((128, 128), F32)],
    )
    mlp = 2 * cells * channels * hidden_units
    forecast, miss, window, normed, inverse, scaled, hidden, preact, rounded = call(
        forward_kernel,
        [
            shape((nfields, cells)),
            shape((nfields, cells)),
            shape((height + 4, width + 16, channels)),
            shape((cells, channels)),
            shape((cells, 1)),
            shape((cells, channels), BF),
            shape((cells, hidden_units), BF),
            shape((cells, hidden_units)),
            shape((cells, channels), BF),
        ],
        (
            field, part, *traded, conv_kernel, gain, up_weight, down_turned, head_turned,
            truth,
        ),
        2 * mlp,
        [pltpu.VMEM((cells, channels), F32)],
    )
    near = [forecast] + [swap(forecast, "mem", 2 * k) for k in order(members // 2)]
    slope, turned = call(
        slope_kernel,
        [shape((cells, hidden_units)), shape((channels, cells), BF)],
        (preact, scaled),
        mlp,
    )
    others = near[1:] + [swap(piece, "mem", 1) for piece in near]
    main_rows = halves * lanes
    half = (main_rows + sum(EXTRA)) // 4
    own, sent, d_output, d_preact = call(
        functools.partial(score_kernel, members, bands, count),
        [
            shape((half, lanes)),
            shape((half, lanes), BF),
            shape((cells, channels)),
            shape((cells, hidden_units), BF),
        ],
        (
            *others, forecast, miss, weights, head_turned, down_turned, rounded, hidden, slope,
            turned,
        ),
        2 * mlp,
        [
            pltpu.VMEM((128, -(-cells // 128) * 128), F32),
            pltpu.VMEM((2, half, lanes), F32),
            pltpu.VMEM((nfields, hidden_units), F32),
            pltpu.VMEM((128, 128), F32),
        ],
    )
    got = send(stages()[0], [sent])
    wide, gain_row = call(
        input_kernel,
        [shape((cells, channels)), shape((1, channels))],
        (d_preact, up_weight, gain, normed, inverse, d_output),
        mlp,
    )
    one = sum_up([(own, *got)], stages()[1])
    first = across_plane(*one)
    own, sent = call(
        rest_kernel,
        [shape((half, lanes)), shape((half, lanes), BF)],
        (
            d_preact, turned, scaled, window, wide, gain_row,
            one[0],
        ),
        2 * mlp,
        [
            pltpu.VMEM((128, lanes + 128), F32),
            pltpu.VMEM((2, half, lanes), F32),
        ],
    )
    two = scatter_start(own, sent)
    second = across_plane(*two)
    one = finish_exchange(first)
    two = finish_exchange(second)
    loss, grad_down, grad_head = call(
        functools.partial(finish_down_kernel, count),
        [shape((1, 1)), shape((channels, hidden_units)), shape((nfields, channels))],
        (*one, field_head_weight),
        mlp // 4,
    )
    grad_kernel, grad_gain, grad_up = call(
        finish_up_kernel,
        [shape(conv_kernel.shape), shape((channels,)), shape(up_weight.shape)],
        (*one, *two),
        mlp // 4,
        [pltpu.VMEM((2, half, lanes), F32)] * 2,
    )
    return (
        loss.reshape(()), grad_kernel, grad_gain, grad_up, grad_down.T, grad_head.T,
    )


def solution(mesh):
    return jax.shard_map(
        local,
        mesh=mesh,
        in_specs=(P("mem", None, "lat", None), P(), P(), P(), P(), P(), P(None, "lat", None), P()),
        out_specs=(P(), P(), P(), P(), P(), P()),
        check_vma=False,
    )
```
